32 devices in a mesh: mem: 4 (over x, core), tile: 8 (over z, y).
Axes of the slice: x: 2, y: 2, z: 4, core: 2. Of those that a mesh axis runs over, the one named last changes fastest.
Arguments:
- alpha: bfloat16 [80, 64, 32, 128], P('mem', 'tile'), may hold values from -0.8984375 to 0.8984375
- ensemble: bfloat16 [80, 3, 64, 32, 128], P('mem', None, 'tile'), may hold values from -6 to 6
- loc_vert: bfloat16 [128, 128], replicated, may hold values from -0.25 to 1.5, as said below
- obs_col: int32 [8, 2048], P('tile'), may hold values from 0 to 1023
- obs_lev: int32 [8, 2048], P('tile'), may hold values from 0 to 127
- obs_count: int32 [8], P('tile'), may hold values from 512 to 2048
- innovation: float32 [8, 2048], P('tile'), may hold values from -6 to 6
- obs_weight: float32 [8, 2048], P('tile'), may hold values from 1 to 8
Outputs:
- gradient: float32 [80, 64, 32, 128], P('mem', 'tile')
The draws below stay inside these ranges and needn't reach their ends.
Inputs may be any that keep to these rules, and one draw needn't show every extreme that they name: `loc_vert`: a square root of the vertical localization, applied along levels.
All inputs are finite; a program needn't handle non-finite values.
Results may differ from the reference program's by a relative error of at most 0.0019.
Values sent between devices are 32-bit elements; how exact they have to be, the bound alone decides.
A program may use at most 64 MiB of HBM per device.

```python
import math
import jax
import jax.numpy as jnp
from jax import lax

V = 3
L = 128
NS = 2
CY = 8
CX = 32
NOBS = 2048
MEMBERS = 80
NYC = 64
TILES = 8


def draw_loc_vert(key, part):
    base = jax.random.fold_in(key, 11)
    first, second = jax.random.split(base)
    diagonal = jax.random.uniform(first, (L,), jnp.float32, 0.5, 1.5)
    others = jax.random.normal(second, (L, L), jnp.float32) * (0.5 / jnp.sqrt(L * 1.0))
    whole = jnp.eye(L, dtype=jnp.float32) * diagonal[None, :] + others
    whole = jnp.clip(whole, -0.25, 1.5)
    return whole.astype(jnp.bfloat16)


def plant(array, key, smallest, high):
    longest = array.shape.index(max(array.shape))
    spots = []
    for shift in (0, 1):
        where = [jax.random.randint(jax.random.fold_in(key, axis), (), 0, length) for axis, length in enumerate(array.shape)]
        where[longest] = (where[longest] + shift) % array.shape[longest]
        spots.append(tuple(where))
    return array.at[spots[0]].set(smallest).at[spots[1]].set(high)


def block_scale(key, extent, pieces, smallest, high):
    def one(position, parts):
        draws = jax.random.uniform(jax.random.fold_in(jax.random.fold_in(key, 6), position), (parts,), jnp.float32, smallest / len(pieces), high / len(pieces))
        return jnp.repeat(jnp.exp(draws), extent[position] // parts).reshape((-1,) + (1,) * (len(extent) - position - 1))

    level = one(*pieces[0])
    for cut in pieces[1:]:
        level = level * one(*cut)
    return level


def normal_values(own_key, shape, width, reach, shards=(), kind=jnp.bfloat16):
    gain = block_scale(own_key, shape, shards, -0.22, 0.18) if shards else 1.0
    drawn = jax.random.normal(own_key, shape, jnp.float32) * width * gain
    return jnp.minimum(jnp.maximum(drawn, -reach), reach).astype(kind)


def setup_inputs(seed: int = 0) -> dict:
    key_of = jax.random.split(jax.random.key(seed), 9)
    alpha = normal_values(key_of[0], (MEMBERS, NYC, CX, L), 0.15, 0.8984375, ((0, 4), (1, 8)))
    ensemble = normal_values(key_of[1], (MEMBERS, V, NYC, CX, L), 1.0, 6.0, ((0, 4), (2, 8)))
    loc_vert = draw_loc_vert(jax.random.fold_in(key_of[8], 71), 0)
    obs_col = plant(jax.random.randint(key_of[3], (TILES, NOBS), 0, 4 * CY * CX), jax.random.fold_in(key_of[3], 1), 0, (4 * CY * CX) - 1).astype(jnp.int32)
    obs_lev = plant(jax.random.randint(key_of[4], (TILES, NOBS), 0, L), jax.random.fold_in(key_of[4], 1), 0, L - 1).astype(jnp.int32)
    obs_count = plant(jax.random.randint(key_of[5], (TILES,), NOBS // 4, NOBS + 1), jax.random.fold_in(key_of[5], 1), NOBS // 4, NOBS).astype(jnp.int32)
    innovation = normal_values(key_of[6], (TILES, NOBS), 1.0, 6.0, ((0, 8),), jnp.float32)
    obs_weight = jnp.clip(jnp.exp(math.log(8.0) - 2.0794415 * jax.random.uniform(key_of[7], (TILES, NOBS), jnp.float32) ** block_scale(key_of[7], (TILES, NOBS), ((0, 8),), -0.2, 0.2)), 1.0, 8.0)
    return dict(alpha=alpha, ensemble=ensemble, loc_vert=loc_vert, obs_col=obs_col, obs_lev=obs_lev, obs_count=obs_count, innovation=innovation, obs_weight=obs_weight)


def widen(field, axis):
    pads = [(1, 1) if dim == axis else (0, 0) for dim in range(field.ndim)]
    return jnp.pad(field, pads)


def spread(padded, axis):
    length = padded.shape[axis] - 2
    before = lax.slice_in_dim(padded, 0, length, axis=axis)
    middle = lax.slice_in_dim(padded, 1, length + 1, axis=axis)
    after = lax.slice_in_dim(padded, 2, length + 2, axis=axis)
    return 0.25 * before + 0.5 * middle + 0.25 * after


def smooth(field, row_axis):
    for sweep in range(NS):
        field = spread(widen(field, row_axis), row_axis)
        field = spread(widen(field, row_axis + 1), row_axis + 1)
    return field


def refine(padded, axis):
    length = padded.shape[axis] - 2
    before = lax.slice_in_dim(padded, 0, length, axis=axis)
    middle = lax.slice_in_dim(padded, 1, length + 1, axis=axis)
    after = lax.slice_in_dim(padded, 2, length + 2, axis=axis)
    evens = 0.75 * middle + 0.25 * before
    odds = 0.75 * middle + 0.25 * after
    stacked = jnp.stack([evens, odds], axis=axis + 1)
    shape = list(middle.shape)
    shape[axis] = 2 * length
    return stacked.reshape(shape)


def coarsen(padded, axis):
    length = padded.shape[axis] - 2
    first = lax.slice_in_dim(padded, 0, length, 2, axis=axis)
    second = lax.slice_in_dim(padded, 1, length + 1, 2, axis=axis)
    third = lax.slice_in_dim(padded, 2, length + 2, 2, axis=axis)
    fourth = lax.slice_in_dim(padded, 3, length + 2, 2, axis=axis)
    return 0.25 * first + 0.75 * second + 0.75 * third + 0.25 * fourth


def reference(alpha, ensemble, loc_vert, obs_col, obs_lev, obs_count, innovation, obs_weight):
    def add_member(running, member_item):
        control, member = member_item
        lifted = smooth(jnp.dot(control, loc_vert.T, preferred_element_type=jnp.float32), 0).astype(jnp.bfloat16)
        return running + member.astype(jnp.float32) * lifted.astype(jnp.float32)[None], 0

    initial = jnp.zeros(ensemble.shape[1:], jnp.float32)
    increment, unused = lax.scan(add_member, initial, (alpha, ensemble))
    fine = refine(widen(refine(widen(increment, 1), 1), 2), 2)
    strips = obs_col.shape[0]
    slots = obs_col.shape[1]
    strip_rows = fine.shape[1] // strips
    fine_width = fine.shape[2]
    variable = jnp.broadcast_to((jnp.arange(slots, dtype=jnp.int32) % V)[None, :], (strips, slots))
    row_index = jnp.arange(strips, dtype=jnp.int32)[:, None] * strip_rows + obs_col // fine_width
    col_index = obs_col % fine_width
    values = fine[variable, row_index, col_index, obs_lev]
    live = jnp.arange(slots, dtype=jnp.int32)[None, :] < obs_count[:, None]
    weighted = jnp.where(live, obs_weight * (values - innovation), jnp.zeros_like(values))
    fine_adjoint = jnp.zeros_like(fine).at[variable, row_index, col_index, obs_lev].add(weighted)
    coarse_adjoint = coarsen(widen(coarsen(widen(fine_adjoint, 2), 2), 1), 1)

    def member_gradient(member_item):
        control, member = member_item
        back = jnp.sum(member.astype(jnp.float32) * coarse_adjoint, axis=0)
        back = smooth(back, 0)
        return control.astype(jnp.float32) + jnp.dot(back, loc_vert.astype(jnp.float32), precision=lax.Precision.HIGHEST)

    return lax.map(member_gradient, (alpha, ensemble))
```

```python
import functools

import jax
import jax.numpy as jnp
from jax import lax
from jax.experimental import pallas as pl
from jax.experimental.pallas import tpu as pltpu
from jax.sharding import PartitionSpec as P

V = 3
F32 = jnp.float32
BF16 = jnp.bfloat16
MESH = pl.DeviceIdType.MESH


def split2(x):
    hi = x.astype(BF16)
    lo = (x - hi.astype(F32)).astype(BF16)
    return hi, lo


def dot(a, b):
    return jnp.dot(a, b, preferred_element_type=F32)


def dot_nt(a, b):
    return lax.dot_general(a, b, (((1,), (1,)), ((), ())), preferred_element_type=F32)


def band(distance):
    d = jnp.abs(distance)
    return jnp.where(d == 0, 6.0, jnp.where(d == 1, 4.0, jnp.where(d == 2, 1.0, 0.0)))


def column_weight(c, c2, cols):
    end = (c == c2) & ((c == 0) | (c == cols - 1))
    return (band(c - c2) - jnp.where(end, 1.0, 0.0)) * (1.0 / 16.0)


def kernel(n, tiles, chunks, alpha_h, ens_h, loc_h, col_h, lev_h, cnt, innov_h, wgt_h, out,
           av, ens, loc, col, lev, innov, wgt,
           hs, hr, hl, gs, gr, gl, mm, sc, em, wt, w15, sent, e15,
           bi, bi1, bi2, fi, b0, b01, b02, f0, b1, b11, b12, f1,
           ihalo, adj, adjs, ahalo, adjs15, ahalo15, gs15, gr15,
           in_sem, hs_s, hs_r, hl_s, hl_r, gs_s, gs_r, gl_s, gl_r,
           sh_s, sh_r, ih_s, ih_r, ah_s, ah_r, a15_s, a15_r, g15_s, g15_r):
    members, rows, cols, levels = out.shape
    size = rows * cols
    ch = cols // 2
    mid = (rows - 4) // 2
    per = members // chunks
    group = 4 if members % 4 == 0 else 1
    slots = col.shape[1]
    m = lax.axis_index("mem")
    t = lax.axis_index("tile")
    p = lax.rem(m, 2)
    mate = m + 1 - 2 * p
    has = (t > 0, t < tiles - 1)
    near = (t - 1, t + 1)
    edge = (slice(0, 2), slice(rows - 2, rows))
    half = (slice(0, ch), slice(ch, cols))

    def loads():
        pairs = (
            (alpha_h.at[:, 0:2], av.at[:, 0:2]),
            (alpha_h.at[:, rows - 2 : rows], av.at[:, rows - 2 : rows]),
            (loc_h, loc),
            (alpha_h.at[:, 2 : rows - 2], av.at[:, 2 : rows - 2]),
            (ens_h, ens),
            (col_h, col), (lev_h, lev), (innov_h, innov), (wgt_h, wgt))
        return [pltpu.make_async_copy(a, b, in_sem.at[i]) for i, (a, b) in enumerate(pairs)]

    copies = loads()
    for copy in copies:
        copy.start()

    relays = tiles % 2 == 0 and tiles >= 4
    odd = lax.rem(t, 2)
    turn = tiles // 2
    share_out = lax.div(chunks * lax.div(t + odd, 2), max(turn, 1))
    n_out = odd * (chunks - share_out) + (1 - odd) * share_out
    share_in = lax.div(chunks * lax.div(t + 2 - 3 * odd, 2), max(turn, 1))
    n_in = (1 - odd) * (chunks - share_in) + odd * share_in
    far = (t >= 2, t <= tiles - 3)
    passes = jnp.where(odd == 1, t - 2, tiles - 3 - t) >= 0

    barrier = pltpu.get_barrier_semaphore()

    def greet(who, where):
        pl.semaphore_signal(barrier, inc=1, device_id={"mem": who, "tile": where}, device_id_type=MESH)

    for d in range(1, n):
        greet(lax.rem(m + d, n), t)
    total = jnp.int32(n - 1)
    for s in range(2):
        @pl.when(has[s])
        def _(s=s):
            greet(m, near[s])
            greet(mate, near[s])
        total = total + 2 * has[s].astype(jnp.int32)
        if relays:
            @pl.when(far[s])
            def _(s=s):
                greet(m, t - 2 + 4 * s)
            total = total + far[s].astype(jnp.int32)

    def remote(src, dst, ssem, rsem, who, where):
        return pltpu.make_async_remote_copy(
            src_ref=src, dst_ref=dst, send_sem=ssem, recv_sem=rsem,
            device_id={"mem": who, "tile": where}, device_id_type=MESH)

    class Halo:
        def __init__(self, src, dst, via, ss, sr, vs, vr):
            self.src, self.dst, self.via = src, dst, via
            self.ss, self.sr, self.vs, self.vr = ss, sr, vs, vr

        def direct(self, h, s, c):
            part = pl.ds(c * per, per)
            return remote(self.src.at[h, s, part], self.dst.at[h, 1 - s, part],
                          self.ss.at[h, s, c], self.sr.at[h, 1 - s, c], m, near[s])

        def detour(self, h, s, c):
            part = pl.ds(c * per, per)
            return remote(self.src.at[h, s, part], self.via.at[h, part],
                          self.ss.at[h, s, c], self.vr.at[h, c], m, t + 1 - 2 * odd)

        def onward(self, h, c):
            part = pl.ds(c * per, per)
            return remote(self.via.at[h, part], self.dst.at[h, odd, part],
                          self.vs.at[h, c], self.sr.at[h, odd, c], m, t + 2 - 4 * odd)

        def send(self, h, c):
            for s in range(2):
                if relays:
                    turned = (odd == s) & (c >= chunks - n_out)

                    @pl.when(has[s] & turned)
                    def _(s=s):
                        self.detour(h, s, c).start()

                    @pl.when(has[s] & jnp.logical_not(turned))
                    def _(s=s):
                        self.direct(h, s, c).start()
                else:
                    @pl.when(has[s])
                    def _(s=s):
                        self.direct(h, s, c).start()

        def forward(self, h, c):
            if relays:
                @pl.when(passes & (c >= chunks - n_in))
                def _():
                    self.onward_recv(h, c).wait_recv()
                    self.onward(h, c).start()

        def onward_recv(self, h, c):
            part = pl.ds(c * per, per)
            return remote(self.via.at[h, part], self.via.at[h, part],
                          self.vs.at[h, c], self.vr.at[h, c], m, t + 1 - 2 * odd)

        def receive(self, h, c):
            for s in range(2):
                @pl.when(has[s])
                def _(s=s):
                    part = pl.ds(c * per, per)
                    remote(self.dst.at[h, s, part], self.dst.at[h, s, part],
                           self.ss.at[h, s, c], self.sr.at[h, s, c], m, near[s]).wait_recv()

        def drain(self):
            for h in range(2):
                for c in range(chunks):
                    for s in range(2):
                        @pl.when(has[s])
                        def _(h=h, s=s, c=c):
                            self.direct(h, s, c).wait_send()
                    if relays:
                        @pl.when(passes & (c >= chunks - n_in))
                        def _(h=h, c=c):
                            self.onward(h, c).wait_send()

    first = Halo(hs, hr, hl, hs_s, hs_r, hl_s, hl_r)
    second = Halo(gs, gr, gl, gs_s, gs_r, gl_s, gl_r)
    order = list(range(chunks - 1, -1, -1))

    i = lax.broadcasted_iota(jnp.int32, (4 * cols, 4 * cols), 0)
    j = lax.broadcasted_iota(jnp.int32, (4 * cols, 4 * cols), 1)
    q, q2 = lax.div(i, cols), lax.div(j, cols)
    across = column_weight(i - q * cols, j - q2 * cols, cols)
    sc[...] = (jnp.where(q == q2, 1.0 / 16.0, 0.0) * across).astype(BF16)
    r = jnp.where(q < 2, q, q + rows - 4)
    r2 = jnp.where(q2 < 2, q2 - 2, q2 - 2 + rows)
    corner = (band(r - r2) * (1.0 / 16.0) * across).astype(BF16)
    em[:, 0 : 4 * cols] = corner
    em[:, 4 * cols :] = corner

    for k in range(3):
        copies[k].wait()
    lv = loc[...]
    lv_nt = jnp.concatenate([lv, lv], axis=1)
    lv_nn = jnp.concatenate([lv, lv], axis=0)

    def prepare(k):
        x = jnp.concatenate([av[k, 0:2], av[k, rows - 2 : rows]], axis=0).reshape(4 * cols, levels)
        both = jnp.concatenate(split2(dot(sc[...], x)), axis=1)
        u = dot_nt(both, lv_nt).reshape(4, cols, levels)
        for s in range(2):
            for h in range(2):
                hs[h, s, k] = u[2 * s : 2 * s + 2, half[h]]

    entered = False
    for c in order:
        for k in range(c * per, (c + 1) * per):
            prepare(k)
        if not entered:
            pl.semaphore_wait(barrier, total)
            entered = True
        first.send(0, c)
    for c in order[: chunks // 2]:
        first.send(1, c)
    for s in range(2):
        @pl.when(jnp.logical_not(has[s]))
        def _(s=s):
            for ref in (hr, gr):
                for h in range(2):
                    ref[h, s] = jnp.zeros(ref.shape[2:], F32)
            for ref in (ihalo, ahalo):
                for h in range(2):
                    ref[h, s] = jnp.zeros(ref.shape[2:], F32)
            ahalo15[s] = jnp.zeros(ahalo15.shape[1:], F32)
            gr15[s] = jnp.zeros(gr15.shape[1:], F32)

    i = lax.broadcasted_iota(jnp.int32, (size, size), 0)
    j = lax.broadcasted_iota(jnp.int32, (size, size), 1)
    r, r2 = lax.div(i, cols), lax.div(j, cols)
    end = (r == r2) & (((r == 0) & (t == 0)) | ((r == rows - 1) & (t == tiles - 1)))
    row_weight = (band(r - r2) - jnp.where(end, 1.0, 0.0)) * (1.0 / 16.0)
    mm[...] = (row_weight * column_weight(i - r * cols, j - r2 * cols, cols)).astype(BF16)

    stage_refs = ((b0, b01, b02, f0), (b1, b11, b12, f1), (bi, bi1, bi2, fi))
    for ref in (b0, b1, bi):
        ref[...] = jnp.zeros_like(ref)
    copies[3].wait()
    copies[4].wait()

    def lift(b, carry):
        ks = [b * group + g for g in range(group)]
        x = jnp.concatenate([av[k].reshape(size, levels) for k in ks], axis=1)
        hi, lo = split2(dot(mm[...], x))
        bases = []
        for g in range(group):
            part = slice(g * levels, (g + 1) * levels)
            both = jnp.concatenate([hi[:, part], lo[:, part]], axis=1)
            bases.append(dot_nt(both, lv_nt).reshape(rows, cols, levels))
        for v in range(V):
            total = ens[ks[0], v].astype(F32) * bases[0]
            for g in range(1, group):
                total = total + ens[ks[g], v].astype(F32) * bases[g]
            for s in range(2):
                bi[s, v] += total[2 + s * mid : 2 + (s + 1) * mid]
                b0[s, v] += total[edge[s], half[0]]
                b1[s, v] += total[edge[s], half[1]]
        return carry

    lax.fori_loop(0, members // group, lift, 0)

    def to_mate(g):
        part, rec, rec2, full = stage_refs[g]
        return remote(part.at[1 - p], rec, sh_s.at[g, 0], sh_r.at[g, 0], mate, t)

    def to_peer(g, d):
        part, rec, rec2, full = stage_refs[g]
        return remote(part.at[p], rec2.at[d - 1], sh_s.at[g, d], sh_r.at[g, d], lax.rem(m + 2 * d, n), t)

    def back_to_mate(g):
        part, rec, rec2, full = stage_refs[g]
        return remote(full.at[p], full.at[p], sh_s.at[g, n // 2], sh_r.at[g, n // 2], mate, t)

    def back_from_mate(g):
        part, rec, rec2, full = stage_refs[g]
        return remote(full.at[1 - p], full.at[1 - p], sh_s.at[g, n // 2], sh_r.at[g, n // 2], mate, t)

    def reduce_chip(g):
        part, rec, rec2, full = stage_refs[g]
        to_mate(g).wait_recv()
        part[p] += rec[...]
        for d in range(1, n // 2):
            to_peer(g, d).start()

    def reduce_rest(g):
        part, rec, rec2, full = stage_refs[g]
        total = part[p]
        for d in range(1, n // 2):
            to_peer(g, d).wait_recv()
            total = total + rec2[d - 1]
        full[p] = total

    def outer_copy(h, s, other):
        full = stage_refs[h][3]
        return remote(full.at[s, :, s], ihalo.at[h, 1 - s], ih_s.at[h, s, other], ih_r.at[h, 1 - s],
                      mate if other else m, near[s])

    def outer_recv(h, s):
        return remote(ihalo.at[h, s], ihalo.at[h, s], ih_s.at[h, s, 0], ih_r.at[h, s], m, near[s])

    def outer_send(h):
        for s in range(2):
            @pl.when(has[s] & (p == s))
            def _(s=s):
                outer_copy(h, s, 0).start()
                outer_copy(h, s, 1).start()

    to_mate(2).start()
    first.forward(0, order[0])
    for k in range(5, 9):
        copies[k].wait()

    place = col[...]
    wide = 2 * cols
    frow = lax.div(place, wide)
    fcol = place - frow * wide
    slot = lax.broadcasted_iota(jnp.int32, (1, slots), 1)
    variable = lax.rem(slot, V)
    early = fcol <= 2 * (ch - 1)
    live = slot < cnt[0]

    def weights(fine, count, shift):
        main = lax.div(fine, 2)
        other = jnp.where(fine - 2 * main == 1, main + 1, main - 1)
        at = lax.broadcasted_iota(jnp.int32, (count, slots), 0) - shift
        return jnp.where(at == main, 0.75, 0.0) + jnp.where(at == other, 0.25, 0.0)

    wr = weights(frow, rows + 2, 1)
    wc = weights(fcol, cols, 0)
    w15[...] = jnp.zeros_like(w15)
    for v in range(V):
        mask = jnp.where(variable == v, 1.0, 0.0)
        for a in range(rows + 2):
            start = (a * V + v) * ch
            line = wr[a : a + 1, :] * mask
            for h in range(2):
                wt[h, start : start + ch, :] = (wc[half[h]] * line).astype(BF16)
            w15[a * V + v : a * V + v + 1, :] = wc[ch - 1 : ch] * line
        if v == 0:
            reduce_chip(2)
    for c in order[1:-1]:
        first.forward(0, c)
    reduce_rest(2)
    back_to_mate(2).start()
    first.forward(0, order[-1])

    e15[...] = jnp.zeros_like(e15)
    for s in range(2):
        for w in range(2):
            row = s * (rows - 2) + w
            for v in range(V):
                for k in range(members):
                    e15[s, w, v, k : k + 1, :] = ens[k, v, row, ch - 1 : ch, :].astype(F32)

    def edge_increment(h, c):
        part = stage_refs[h][0]
        sums = [[None] * V for _ in range(2)]
        for k in range(c * per, (c + 1) * per):
            above, below = hr[h, 0, k], hr[h, 1, k]
            fields = (jnp.stack([above[0] + 4.0 * above[1], above[1]]),
                      jnp.stack([below[0], 4.0 * below[0] + below[1]]))
            for s in range(2):
                for v in range(V):
                    term = ens[k, v, edge[s], half[h]].astype(F32) * fields[s]
                    sums[s][v] = term if sums[s][v] is None else sums[s][v] + term
        for s in range(2):
            for v in range(V):
                part[s, v] += sums[s][v]

    def whole(h):
        full = stage_refs[h][3]
        pieces = [ihalo[h, 0], full[0, :, 0], full[0, :, 1]]
        pieces += [fi[s, :, a, half[h]] for s in range(2) for a in range(mid)]
        pieces += [full[1, :, 0], full[1, :, 1], ihalo[h, 1]]
        return jnp.concatenate(pieces, axis=0).reshape(V * (rows + 2) * ch, levels)

    hot = lax.broadcasted_iota(jnp.int32, (levels, slots), 0) == lev[...]

    def pick(h):
        both = jnp.concatenate(split2(whole(h).T), axis=0)
        picked = dot(both, wt[h])
        return jnp.sum(jnp.where(hot, picked[:levels] + picked[levels:], 0.0), axis=0, keepdims=True)

    def spread(weighted):
        hi, lo = split2(jnp.where(hot, jnp.broadcast_to(weighted, hot.shape), 0.0))
        sent[0:levels, :] = hi
        sent[levels:, :] = lo

    def adjoint(h, a, count):
        both = dot_nt(wt[h, a * V * ch : (a + count) * V * ch, :], sent[...])
        return (both[:, :levels] + both[:, levels:]).reshape(count, V, ch, levels)

    def near_copy(src, dst, ssem, rsem, h, s):
        return remote(src.at[h, s], dst.at[h, 1 - s], ssem.at[h, s], rsem.at[h, 1 - s], m, near[s])

    def single_copy(src, dst, ssem, rsem, s):
        return remote(src.at[s], dst.at[1 - s], ssem.at[s], rsem.at[1 - s], m, near[s])

    def adjoint_edges(h):
        top, bottom = adjoint(h, 0, 3), adjoint(h, rows - 1, 3)
        adjs[h, 0] = top[0]
        adjs[h, 1] = bottom[2]
        for s in range(2):
            @pl.when(has[s])
            def _(s=s):
                near_copy(adjs, ahalo, ah_s, ah_r, h, s).start()
        for a in range(2):
            adj[:, a, half[h]] = top[1 + a]
            adj[:, rows - 2 + a, half[h]] = bottom[a]

    def adjoint_halo(h):
        for s in range(2):
            @pl.when(has[s])
            def _(s=s):
                remote(ahalo.at[h, s], ahalo.at[h, s], ah_s.at[h, s], ah_r.at[h, s], m, near[s]).wait_recv()
        adj[:, 0, half[h]] += ahalo[h, 0]
        adj[:, rows - 1, half[h]] += ahalo[h, 1]

    def fields(h, c):
        weights = [[adj[v, edge[s], half[h]] for v in range(V)] for s in range(2)]
        for k in range(c * per, (c + 1) * per):
            for s in range(2):
                total = ens[k, 0, edge[s], half[h]].astype(F32) * weights[s][0]
                for v in range(1, V):
                    total = total + ens[k, v, edge[s], half[h]].astype(F32) * weights[s][v]
                gs[h, s, k] = total

    def chain_sums(h, middle, later):
        to_mate(h).start()
        middle()
        reduce_chip(h)
        reduce_rest(h)
        back_to_mate(h).start()
        outer_send(h)
        later()

    def chain_close(h):
        back_from_mate(h).wait_recv()
        for s in range(2):
            @pl.when(has[s])
            def _(s=s):
                outer_recv(h, s).wait_recv()

    for c in order:
        first.receive(0, c)
        edge_increment(0, c)
    rest = order[chunks // 2 :]

    def after_outer_a():
        for c in rest[:1]:
            first.send(1, c)
        first.forward(1, order[0])

    chain_sums(0, lambda: None, after_outer_a)
    back_from_mate(2).wait_recv()
    chain_close(0)
    value = pick(0)
    weighted = jnp.where(live & early, wgt[...] * (value - innov[...]), 0.0)
    spread(weighted)
    adjoint_edges(0)
    for c in rest[1:]:
        first.send(1, c)
    for c in order[1:]:
        first.forward(1, c)
    adjoint_halo(0)
    for c in order:
        fields(0, c)
        second.send(0, c)

    for c in order:
        first.receive(1, c)
        edge_increment(1, c)
    chain_sums(1, lambda: None, lambda: second.forward(0, order[0]))
    chain_close(1)
    value = value + pick(1)
    spread(jnp.where(live, wgt[...] * (value - innov[...]), 0.0))
    adjoint_edges(1)
    thin = dot_nt(w15[...].astype(BF16), sent[...])
    thin = thin[:, :levels] + thin[:, levels:]
    adjs15[0, 0:V] = thin[0:V]
    adjs15[1, 0:V] = thin[(rows + 1) * V : (rows + 2) * V]
    for s in range(2):
        @pl.when(has[s])
        def _(s=s):
            single_copy(adjs15, ahalo15, a15_s, a15_r, s).start()
    for c in order[1:]:
        second.forward(0, c)
    adjoint_halo(1)
    for s in range(2):
        @pl.when(has[s])
        def _(s=s):
            remote(ahalo15.at[s], ahalo15.at[s], a15_s.at[s], a15_r.at[s], m, near[s]).wait_recv()
    for s in range(2):
        for w in range(2):
            a = 1 + s * (rows - 2) + w
            line = thin[a * V : (a + 1) * V]
            if w == s:
                line = line + ahalo15[s, 0:V]
            total = e15[s, w, 0] * line[0:1]
            for v in range(1, V):
                total = total + e15[s, w, v] * line[v : v + 1]
            gs15[s, w] = total
            for v in range(V):
                adj[v, s * (rows - 2) + w, ch - 1 : ch, :] = line[v : v + 1]
    for c in order:
        fields(1, c)
        second.send(1, c)
        if c == order[0]:
            for s in range(2):
                @pl.when(has[s])
                def _(s=s):
                    single_copy(gs15, gr15, g15_s, g15_r, s).start()
    for h in range(2):
        inner = adjoint(h, 3, rows - 4)
        for a in range(rows - 4):
            adj[:, 2 + a, half[h]] = inner[a]

    pair = 2 if members % 2 == 0 else 1

    def inside(b, carry):
        ks = [b * pair + g for g in range(pair)]
        parts = []
        for k in ks:
            total = ens[k, 0].astype(F32) * adj[0]
            for v in range(1, V):
                total = total + ens[k, v].astype(F32) * adj[v]
            parts.append(total.reshape(size, levels))
        hi, lo = split2(jnp.concatenate(parts, axis=1))
        hi, lo = split2(dot(mm[...], hi) + dot(mm[...], lo))
        for g, k in enumerate(ks):
            part = slice(g * levels, (g + 1) * levels)
            both = jnp.concatenate([hi[:, part], lo[:, part]], axis=1)
            out[k] = av[k].astype(F32) + dot(both, lv_nn).reshape(rows, cols, levels)
        return carry

    first_pairs = (members // pair) // 2
    lax.fori_loop(0, first_pairs, inside, 0)
    for c in order:
        second.forward(1, c)
    lax.fori_loop(first_pairs, members // pair, inside, 0)

    for c in order:
        second.receive(0, c)
    for s in range(2):
        @pl.when(has[s])
        def _(s=s):
            remote(gr15.at[s], gr15.at[s], g15_s.at[s], g15_r.at[s], m, near[s]).wait_recv()

    def outer(k):
        sides = []
        for s in range(2):
            body = jnp.concatenate([gr[0, s, k], gr[1, s, k]], axis=1)
            at = lax.broadcasted_iota(jnp.int32, body.shape, 1)
            line = jnp.stack([gr15[s, w, k : k + 1] for w in range(2)])
            sides.append(jnp.where(at == ch - 1, jnp.broadcast_to(line, body.shape), body))
        around = jnp.concatenate(sides, axis=0).reshape(4 * cols, levels)
        back = dot(em[...], jnp.concatenate(split2(around), axis=0))
        both = jnp.concatenate(split2(back), axis=1)
        add = dot(both, lv_nn).reshape(4, cols, levels)
        out[k, 0:2] += add[0:2]
        out[k, rows - 2 : rows] += add[2:4]

    for c in order:
        second.receive(1, c)
        for k in range(c * per, (c + 1) * per):
            outer(k)

    first.drain()
    second.drain()
    for g in range(3):
        to_mate(g).wait_send()
        for d in range(1, n // 2):
            to_peer(g, d).wait_send()
        back_to_mate(g).wait_send()
    for h in range(2):
        for s in range(2):
            @pl.when(has[s] & (p == s))
            def _(h=h, s=s):
                outer_copy(h, s, 0).wait_send()
                outer_copy(h, s, 1).wait_send()

            @pl.when(has[s])
            def _(h=h, s=s):
                near_copy(adjs, ahalo, ah_s, ah_r, h, s).wait_send()
    for s in range(2):
        @pl.when(has[s])
        def _(s=s):
            single_copy(adjs15, ahalo15, a15_s, a15_r, s).wait_send()
            single_copy(gs15, gr15, g15_s, g15_r, s).wait_send()


def solution(mesh):
    n = mesh.shape["mem"]
    tiles = mesh.shape["tile"]

    def on_device(alpha, ensemble, loc_vert, obs_col, obs_lev, obs_count, innovation, obs_weight):
        members, rows, cols, levels = alpha.shape
        slots = obs_col.shape[1]
        chunks = 4 if members % 4 == 0 else 1
        ch = cols // 2
        mid = (rows - 4) // 2
        vmem = pl.BlockSpec(memory_space=pltpu.VMEM)
        hbm = pl.BlockSpec(memory_space=pltpu.HBM)
        turned = pltpu.VMEM((2, 2, members, 2, ch, levels), F32)
        passing = pltpu.VMEM((2, members, 2, ch, levels), F32)
        dma = pltpu.SemaphoreType.DMA
        line = pltpu.VMEM((1, slots), F32)
        mark = pltpu.VMEM((1, slots), jnp.int32)
        padded = -(-members // 8) * 8
        thin = -(-V * (rows + 2) // 16) * 16

        def sums(piece):
            return [pltpu.VMEM((2,) + piece, F32), pltpu.VMEM(piece, F32),
                    pltpu.VMEM((max(n // 2 - 1, 1),) + piece, F32), pltpu.VMEM((2,) + piece, F32)]

        borders = pltpu.VMEM((2, 2, V, ch, levels), F32)
        small = pltpu.VMEM((2, 8, levels), F32)
        slim = pltpu.VMEM((2, 2, padded, levels), F32)
        return pl.pallas_call(
            functools.partial(kernel, n, tiles, chunks),
            out_shape=jax.ShapeDtypeStruct(alpha.shape, F32),
            in_specs=[hbm, hbm, hbm, hbm, hbm, pl.BlockSpec(memory_space=pltpu.SMEM), hbm, hbm],
            out_specs=vmem,
            scratch_shapes=[
                pltpu.VMEM(alpha.shape, BF16), pltpu.VMEM(ensemble.shape, BF16),
                pltpu.VMEM(loc_vert.shape, BF16), mark, mark, line, line,
                turned, turned, passing, turned, turned, passing,
                pltpu.VMEM((rows * cols, rows * cols), BF16),
                pltpu.VMEM((4 * cols, 4 * cols), BF16),
                pltpu.VMEM((4 * cols, 8 * cols), BF16),
                pltpu.VMEM((2, V * (rows + 2) * ch, slots), BF16),
                pltpu.VMEM((thin, slots), F32),
                pltpu.VMEM((2 * levels, slots), BF16),
                pltpu.VMEM((2, 2, V, padded, levels), F32),
                *sums((V, mid, cols, levels)), *sums((V, 2, ch, levels)), *sums((V, 2, ch, levels)),
                borders, pltpu.VMEM((V, rows, cols, levels), F32), borders, borders,
                small, small, slim, slim,
                dma((9,)),
                dma((2, 2, chunks)), dma((2, 2, chunks)), dma((2, chunks)), dma((2, chunks)),
                dma((2, 2, chunks)), dma((2, 2, chunks)), dma((2, chunks)), dma((2, chunks)),
                dma((3, n // 2 + 1)), dma((3, n // 2 + 1)),
                dma((2, 2, 2)), dma((2, 2)), dma((2, 2)), dma((2, 2)),
                dma((2,)), dma((2,)), dma((2,)), dma((2,)),
            ],
            compiler_params=pltpu.CompilerParams(
                collective_id=0, has_side_effects=True, vmem_limit_bytes=58 << 20),
        )(alpha, ensemble, loc_vert, obs_col, obs_lev, obs_count, innovation, obs_weight)

    in_specs = (
        P("mem", "tile", None, None),
        P("mem", None, "tile", None, None),
        P(),
        P("tile", None),
        P("tile", None),
        P("tile"),
        P("tile", None),
        P("tile", None),
    )
    out_specs = P("mem", "tile", None, None)
    return jax.shard_map(
        on_device, mesh=mesh, in_specs=in_specs, out_specs=out_specs, check_vma=False
    )
```

```python
import functools

import jax
import jax.numpy as jnp
from jax import lax
from jax.experimental import pallas as pl
from jax.experimental.pallas import tpu as pltpu
from jax.sharding import PartitionSpec as P

V = 3
F32 = jnp.float32
BF16 = jnp.bfloat16
MESH = pl.DeviceIdType.MESH


def split2(x):
    hi = x.astype(BF16)
    lo = (x - hi.astype(F32)).astype(BF16)
    return hi, lo


def dot(a, b):
    return jnp.dot(a, b, preferred_element_type=F32)


def dot_nt(a, b):
    return lax.dot_general(a, b, (((1,), (1,)), ((), ())), preferred_element_type=F32)


def band(distance):
    d = jnp.abs(distance)
    return jnp.where(d == 0, 6.0, jnp.where(d == 1, 4.0, jnp.where(d == 2, 1.0, 0.0)))


def column_weight(c, c2, cols):
    end = (c == c2) & ((c == 0) | (c == cols - 1))
    return (band(c - c2) - jnp.where(end, 1.0, 0.0)) * (1.0 / 16.0)


def kernel(n, tiles, chunks, alpha_h, ens_h, loc_h, col_h, lev_h, cnt, innov_h, wgt_h, out,
           av, ens, loc, col, lev, innov, wgt,
           hs, hr, hl, gs, gr, gl, mm, sc, em, wt, w15, sent, e15,
           bi, bi1, bi2, fi, b0, b01, b02, f0, b1, b11, b12, f1,
           iy, adj, adjs, ahalo, adjs15, ahalo15, gs15, gr15,
           in_sem, hs_s, hs_r, hl_s, hl_r, gs_s, gs_r, gl_s, gl_r,
           sh_s, sh_r, ih_s, ih_r, ah_s, ah_r, a15_s, a15_r, g15_s, g15_r):
    members, rows, cols, levels = out.shape
    size = rows * cols
    ch = cols // 2
    mid = (rows - 4) // 2
    per = members // chunks
    group = 4 if members % 4 == 0 else 1
    slots = col.shape[1]
    m = lax.axis_index("mem")
    t = lax.axis_index("tile")
    p = lax.rem(m, 2)
    mate = m + 1 - 2 * p
    has = (t > 0, t < tiles - 1)
    near = (t - 1, t + 1)
    edge = (slice(0, 2), slice(rows - 2, rows))
    half = (slice(0, ch), slice(ch, cols))

    def loads():
        pairs = (
            (alpha_h.at[:, 0:2], av.at[:, 0:2]),
            (alpha_h.at[:, rows - 2 : rows], av.at[:, rows - 2 : rows]),
            (loc_h, loc),
            (alpha_h.at[:, 2 : rows - 2], av.at[:, 2 : rows - 2]),
            (ens_h, ens),
            (col_h, col), (lev_h, lev), (innov_h, innov), (wgt_h, wgt))
        return [pltpu.make_async_copy(a, b, in_sem.at[i]) for i, (a, b) in enumerate(pairs)]

    copies = loads()
    for copy in copies:
        copy.start()

    relays = tiles % 2 == 0 and tiles >= 4
    odd = lax.rem(t, 2)
    turn = tiles // 2
    share_out = lax.div(chunks * lax.div(t + odd, 2), max(turn, 1))
    n_out = odd * (chunks - share_out) + (1 - odd) * share_out
    share_in = lax.div(chunks * lax.div(t + 2 - 3 * odd, 2), max(turn, 1))
    n_in = (1 - odd) * (chunks - share_in) + odd * share_in
    far = (t >= 2, t <= tiles - 3)
    passes = jnp.where(odd == 1, t - 2, tiles - 3 - t) >= 0

    barrier = pltpu.get_barrier_semaphore()

    def greet(who, where):
        pl.semaphore_signal(barrier, inc=1, device_id={"mem": who, "tile": where}, device_id_type=MESH)

    for d in range(1, n):
        greet(lax.rem(m + d, n), t)
    total = jnp.int32(n - 1)
    for s in range(2):
        @pl.when(has[s])
        def _(s=s):
            for d in range(n // 2):
                greet(lax.rem(m + 2 * d, n), near[s])
        total = total + (n // 2) * has[s].astype(jnp.int32)
        if relays:
            @pl.when(far[s])
            def _(s=s):
                greet(m, t - 2 + 4 * s)
            total = total + far[s].astype(jnp.int32)

    def remote(src, dst, ssem, rsem, who, where):
        return pltpu.make_async_remote_copy(
            src_ref=src, dst_ref=dst, send_sem=ssem, recv_sem=rsem,
            device_id={"mem": who, "tile": where}, device_id_type=MESH)

    class Halo:
        def __init__(self, src, dst, via, ss, sr, vs, vr):
            self.src, self.dst, self.via = src, dst, via
            self.ss, self.sr, self.vs, self.vr = ss, sr, vs, vr

        def direct(self, h, s, c):
            part = pl.ds(c * per, per)
            return remote(self.src.at[h, s, part], self.dst.at[h, 1 - s, part],
                          self.ss.at[h, s, c], self.sr.at[h, 1 - s, c], m, near[s])

        def detour(self, h, s, c):
            part = pl.ds(c * per, per)
            return remote(self.src.at[h, s, part], self.via.at[h, part],
                          self.ss.at[h, s, c], self.vr.at[h, c], m, t + 1 - 2 * odd)

        def onward(self, h, c):
            part = pl.ds(c * per, per)
            return remote(self.via.at[h, part], self.dst.at[h, odd, part],
                          self.vs.at[h, c], self.sr.at[h, odd, c], m, t + 2 - 4 * odd)

        def send_turned(self, h, c):
            for s in range(2):
                if relays:
                    @pl.when(has[s] & (odd == s) & (c >= chunks - n_out))
                    def _(s=s):
                        self.detour(h, s, c).start()

        def send_far(self, h, c):
            for s in range(2):
                straight = c < chunks - n_out if relays else True

                @pl.when(has[s] & (odd == s) & straight)
                def _(s=s):
                    self.direct(h, s, c).start()

        def send_near(self, h, c):
            for s in range(2):
                @pl.when(has[s] & (odd != s))
                def _(s=s):
                    self.direct(h, s, c).start()

        def send(self, h):
            for c in order:
                self.send_turned(h, c)
            for c in order:
                self.send_far(h, c)
                self.send_near(h, c)

        def forward(self, h, c):
            if relays:
                @pl.when(passes & (c >= chunks - n_in))
                def _():
                    self.onward_recv(h, c).wait_recv()
                    self.onward(h, c).start()

        def onward_recv(self, h, c):
            part = pl.ds(c * per, per)
            return remote(self.via.at[h, part], self.via.at[h, part],
                          self.vs.at[h, c], self.vr.at[h, c], m, t + 1 - 2 * odd)

        def receive(self, h, c):
            for s in range(2):
                @pl.when(has[s])
                def _(s=s):
                    part = pl.ds(c * per, per)
                    remote(self.dst.at[h, s, part], self.dst.at[h, s, part],
                           self.ss.at[h, s, c], self.sr.at[h, s, c], m, near[s]).wait_recv()

        def drain(self):
            for h in range(self.src.shape[0]):
                for c in range(chunks):
                    for s in range(2):
                        @pl.when(has[s])
                        def _(h=h, s=s, c=c):
                            self.direct(h, s, c).wait_send()
                    if relays:
                        @pl.when(passes & (c >= chunks - n_in))
                        def _(h=h, c=c):
                            self.onward(h, c).wait_send()

    first = Halo(hs, hr, hl, hs_s, hs_r, hl_s, hl_r)
    second = Halo(gs, gr, gl, gs_s, gs_r, gl_s, gl_r)
    order = list(range(chunks - 1, -1, -1))

    i = lax.broadcasted_iota(jnp.int32, (4 * cols, 4 * cols), 0)
    j = lax.broadcasted_iota(jnp.int32, (4 * cols, 4 * cols), 1)
    q, q2 = lax.div(i, cols), lax.div(j, cols)
    across = column_weight(i - q * cols, j - q2 * cols, cols)
    sc[...] = (jnp.where(q == q2, 1.0 / 16.0, 0.0) * across).astype(BF16)
    r = jnp.where(q < 2, q, q + rows - 4)
    r2 = jnp.where(q2 < 2, q2 - 2, q2 - 2 + rows)
    corner = (band(r - r2) * (1.0 / 16.0) * across).astype(BF16)
    em[:, 0 : 4 * cols] = corner
    em[:, 4 * cols :] = corner

    for k in range(3):
        copies[k].wait()
    lv = loc[...]
    lv_nt = jnp.concatenate([lv, lv], axis=1)
    lv_nn = jnp.concatenate([lv, lv], axis=0)

    def prepare(k):
        x = jnp.concatenate([av[k, 0:2], av[k, rows - 2 : rows]], axis=0).reshape(4 * cols, levels)
        both = jnp.concatenate(split2(dot(sc[...], x)), axis=1)
        u = dot_nt(both, lv_nt).reshape(4, cols, levels)
        for s in range(2):
            for h in range(2):
                hs[h, s, k] = u[2 * s : 2 * s + 2, half[h]]

    entered = False
    for c in order:
        for k in range(c * per, (c + 1) * per):
            prepare(k)
        if not entered:
            pl.semaphore_wait(barrier, total)
            entered = True
        first.send_turned(0, c)
        first.send_far(0, c)
    for c in order:
        first.send_near(0, c)
    for c in order:
        first.send_turned(1, c)
    for s in range(2):
        @pl.when(jnp.logical_not(has[s]))
        def _(s=s):
            for ref in (hr, gr, ahalo):
                for h in range(ref.shape[0]):
                    ref[h, s] = jnp.zeros(ref.shape[2:], F32)
            ahalo15[s] = jnp.zeros(ahalo15.shape[1:], F32)
            gr15[s] = jnp.zeros(gr15.shape[1:], F32)

    i = lax.broadcasted_iota(jnp.int32, (size, size), 0)
    j = lax.broadcasted_iota(jnp.int32, (size, size), 1)
    r, r2 = lax.div(i, cols), lax.div(j, cols)
    end = (r == r2) & (((r == 0) & (t == 0)) | ((r == rows - 1) & (t == tiles - 1)))
    row_weight = (band(r - r2) - jnp.where(end, 1.0, 0.0)) * (1.0 / 16.0)
    mm[...] = (row_weight * column_weight(i - r * cols, j - r2 * cols, cols)).astype(BF16)

    stage_refs = ((b0, b01, b02, f0), (b1, b11, b12, f1), (bi, bi1, bi2, fi))
    for ref in (b0, b1, bi):
        ref[...] = jnp.zeros_like(ref)
    copies[3].wait()
    copies[4].wait()

    def lift(b, carry):
        ks = [b * group + g for g in range(group)]
        x = jnp.concatenate([av[k].reshape(size, levels) for k in ks], axis=1)
        hi, lo = split2(dot(mm[...], x))
        bases = []
        for g in range(group):
            part = slice(g * levels, (g + 1) * levels)
            both = jnp.concatenate([hi[:, part], lo[:, part]], axis=1)
            bases.append(dot_nt(both, lv_nt).reshape(rows, cols, levels))
        for v in range(V):
            total = ens[ks[0], v].astype(F32) * bases[0]
            for g in range(1, group):
                total = total + ens[ks[g], v].astype(F32) * bases[g]
            for s in range(2):
                bi[s, v] += total[2 + s * mid : 2 + (s + 1) * mid]
                b0[s, v] += total[edge[s], half[0]]
                b1[s, v] += total[edge[s], half[1]]
        return carry

    lax.fori_loop(0, members // group, lift, 0)

    def to_mate(g):
        part, rec, rec2, full = stage_refs[g]
        return remote(part.at[1 - p], rec, sh_s.at[g, 0], sh_r.at[g, 0], mate, t)

    def to_peer(g, d):
        part, rec, rec2, full = stage_refs[g]
        return remote(part.at[p], rec2.at[d - 1], sh_s.at[g, d], sh_r.at[g, d], lax.rem(m + 2 * d, n), t)

    def back_to_mate(g):
        part, rec, rec2, full = stage_refs[g]
        return remote(full.at[p], full.at[p], sh_s.at[g, n // 2], sh_r.at[g, n // 2], mate, t)

    def back_from_mate(g):
        part, rec, rec2, full = stage_refs[g]
        return remote(full.at[1 - p], full.at[1 - p], sh_s.at[g, n // 2], sh_r.at[g, n // 2], mate, t)

    def reduce_chip(g):
        part, rec, rec2, full = stage_refs[g]
        to_mate(g).wait_recv()
        part[p] += rec[...]
        for d in range(1, n // 2):
            to_peer(g, d).start()

    def reduce_rest(g):
        part, rec, rec2, full = stage_refs[g]
        total = part[p]
        for d in range(1, n // 2):
            to_peer(g, d).wait_recv()
            total = total + rec2[d - 1]
        return total

    def outer_copy(h, s, d):
        here = lax.div(m, 2)
        return remote(stage_refs[h][0].at[p, :, s], iy.at[h, here], ih_s.at[h, d], ih_r.at[h, here],
                      lax.rem(m + 2 * d, n), near[s])

    def outer_send(h):
        for s in range(2):
            @pl.when(has[s] & (p == s))
            def _(s=s):
                for d in range(n // 2):
                    outer_copy(h, s, d).start()

    def outer_recv(h):
        full = stage_refs[h][3]
        for s in range(2):
            @pl.when(has[1 - s] & (p == s))
            def _(s=s):
                total = None
                for d in range(n // 2):
                    remote(iy.at[h, d], iy.at[h, d], ih_s.at[h, 0], ih_r.at[h, d], m, near[1 - s]).wait_recv()
                    total = iy[h, d] if total is None else total + iy[h, d]
                full[s, :, 2] = total

            @pl.when(jnp.logical_not(has[1 - s]) & (p == s))
            def _(s=s):
                full[s, :, 2] = jnp.zeros(full.shape[1:2] + full.shape[3:], F32)

    to_mate(2).start()
    first.forward(0, order[0])
    for k in range(5, 9):
        copies[k].wait()

    place = col[...]
    wide = 2 * cols
    frow = lax.div(place, wide)
    fcol = place - frow * wide
    slot = lax.broadcasted_iota(jnp.int32, (1, slots), 1)
    variable = lax.rem(slot, V)
    early = fcol <= 2 * (ch - 1)
    live = slot < cnt[0]

    def weights(fine, count, shift):
        main = lax.div(fine, 2)
        other = jnp.where(fine - 2 * main == 1, main + 1, main - 1)
        at = lax.broadcasted_iota(jnp.int32, (count, slots), 0) - shift
        return jnp.where(at == main, 0.75, 0.0) + jnp.where(at == other, 0.25, 0.0)

    wr = weights(frow, rows + 2, 1)
    wc = weights(fcol, cols, 0)
    head = w15.shape[0]
    w15[...] = jnp.zeros_like(w15)
    rim = [0, 1, 2, rows - 1, rows, rows + 1]
    lines = rim + list(range(3, rows - 1))
    cut = head + len(rim) * V * ch
    for v in range(V):
        mask = jnp.where(variable == v, 1.0, 0.0)
        for b, a in enumerate(lines):
            start = head + (b * V + v) * ch
            line = wr[a : a + 1, :] * mask
            for h in range(2):
                wt[h, start : start + ch, :] = (wc[half[h]] * line).astype(BF16)
            if b < len(rim):
                w15[b * V + v : b * V + v + 1, :] = wc[ch - 1 : ch] * line
        if v == 0:
            reduce_chip(2)
    wt[1, 0:head, :] = w15[...].astype(BF16)
    for c in order:
        first.send_far(1, c)
    for c in order[1:2]:
        first.forward(0, c)
    fi[p] = reduce_rest(2)
    back_to_mate(2).start()

    e15[...] = jnp.zeros_like(e15)
    for s in range(2):
        for w in range(2):
            row = s * (rows - 2) + w
            for v in range(V):
                for k in range(members):
                    e15[s, w, v, k : k + 1, :] = ens[k, v, row, ch - 1 : ch, :].astype(F32)

    def edge_increment(h, c):
        part = stage_refs[h][0]
        sums = [[None] * V for _ in range(2)]
        for k in range(c * per, (c + 1) * per):
            above, below = hr[h, 0, k], hr[h, 1, k]
            fields = (jnp.stack([above[0] + 4.0 * above[1], above[1]]),
                      jnp.stack([below[0], 4.0 * below[0] + below[1]]))
            for s in range(2):
                for v in range(V):
                    term = ens[k, v, edge[s], half[h]].astype(F32) * fields[s]
                    sums[s][v] = term if sums[s][v] is None else sums[s][v] + term
        for s in range(2):
            for v in range(V):
                part[s, v] += sums[s][v]

    hot = lax.broadcasted_iota(jnp.int32, (levels, slots), 0) == lev[...]

    def pick(h, pieces, start):
        flat = jnp.concatenate(pieces, axis=0).reshape(-1, levels)
        both = jnp.concatenate(split2(flat.T), axis=0)
        picked = dot(both, wt[h, start : start + flat.shape[0]])
        return jnp.sum(jnp.where(hot, picked[:levels] + picked[levels:], 0.0), axis=0, keepdims=True)

    def pick_inner(h):
        return pick(h, [fi[s, :, a, half[h]] for s in range(2) for a in range(mid)], cut)

    def pick_rim(h):
        full = stage_refs[h][3]
        return pick(h, [full[1, :, 2], full[0, :, 0], full[0, :, 1], full[1, :, 0], full[1, :, 1], full[0, :, 2]], head)

    def spread(weighted):
        hi, lo = split2(jnp.where(hot, jnp.broadcast_to(weighted, hot.shape), 0.0))
        sent[0:levels, :] = hi
        sent[levels:, :] = lo

    def adjoint(h, start, stop):
        both = dot_nt(wt[h, start:stop, :], sent[...])
        return both[:, :levels] + both[:, levels:]

    def shaped(x):
        return x.reshape(x.shape[0] // (V * ch), V, ch, levels)

    def near_copy(src, dst, ssem, rsem, h, s):
        return remote(src.at[h, s], dst.at[h, 1 - s], ssem.at[h, s], rsem.at[h, 1 - s], m, near[s])

    def single_copy(src, dst, ssem, rsem, s):
        return remote(src.at[s], dst.at[1 - s], ssem.at[s], rsem.at[1 - s], m, near[s])

    def adjoint_edges(h):
        flat = adjoint(h, head * (1 - h), cut)
        thin = flat[:head] if h else None
        rims = shaped(flat[head * h :])
        adjs[h, 0] = rims[0]
        adjs[h, 1] = rims[5]
        if h:
            adjs15[0, 0:V] = thin[0:V]
            adjs15[1, 0:V] = thin[5 * V : 6 * V]
        for s in range(2):
            @pl.when(has[s])
            def _(s=s):
                near_copy(adjs, ahalo, ah_s, ah_r, h, s).start()
                if h:
                    single_copy(adjs15, ahalo15, a15_s, a15_r, s).start()
        for a in range(2):
            adj[:, a, half[h]] = rims[1 + a]
            adj[:, rows - 2 + a, half[h]] = rims[3 + a]
        return thin

    def adjoint_halo(h):
        for s in range(2):
            @pl.when(has[s])
            def _(s=s):
                remote(ahalo.at[h, s], ahalo.at[h, s], ah_s.at[h, s], ah_r.at[h, s], m, near[s]).wait_recv()
        adj[:, 0, half[h]] += ahalo[h, 0]
        adj[:, rows - 1, half[h]] += ahalo[h, 1]

    def fields(h, outermost):
        where = (0, rows - 1) if outermost else (1, rows - 2)
        weights = [[adj[v, where[s], half[h]] for v in range(V)] for s in range(2)]
        for k in range(members):
            for s in range(2):
                total = ens[k, 0, where[s], half[h]].astype(F32) * weights[s][0]
                for v in range(1, V):
                    total = total + ens[k, v, where[s], half[h]].astype(F32) * weights[s][v]
                gs[2 * h + outermost, s, k] = total

    def chain_open(h):
        for c in order:
            first.receive(h, c)
            edge_increment(h, c)
        to_mate(h).start()
        reduce_chip(h)
        outer_send(h)

    def chain_close(h):
        full = stage_refs[h][3]
        full[p, :, 0:2] = reduce_rest(h)
        outer_recv(h)
        back_to_mate(h).start()
        back_from_mate(h).wait_recv()

    back_from_mate(2).wait_recv()
    value = pick_inner(0)
    for c in order[2:]:
        first.forward(0, c)
    value = value + pick_inner(1)

    chain_open(0)
    for c in order:
        first.send_near(1, c)
    chain_close(0)
    for c in order[:2]:
        first.forward(1, c)
    value = value + pick_rim(0)
    weighted = jnp.where(live & early, wgt[...] * (value - innov[...]), 0.0)
    spread(weighted)
    adjoint_edges(0)
    fields(0, 0)
    second.send(0)
    for c in order[2:]:
        first.forward(1, c)

    chain_open(1)
    adjoint_halo(0)
    fields(0, 1)
    second.send(1)
    for c in order:
        second.forward(0, c)
    chain_close(1)
    value = value + pick_rim(1)
    spread(jnp.where(live, wgt[...] * (value - innov[...]), 0.0))
    thin = adjoint_edges(1)
    fields(1, 0)
    second.send(2)
    for c in order:
        second.forward(1, c)
    for h in range(2):
        inner = shaped(adjoint(h, cut, wt.shape[1]))
        for a in range(rows - 4):
            adj[:, 2 + a, half[h]] = inner[a]
    adjoint_halo(1)
    fields(1, 1)
    second.send(3)
    for s in range(2):
        @pl.when(has[s])
        def _(s=s):
            remote(ahalo15.at[s], ahalo15.at[s], a15_s.at[s], a15_r.at[s], m, near[s]).wait_recv()
    for s in range(2):
        for w in range(2):
            a = 1 + 2 * s + w
            line = thin[a * V : (a + 1) * V]
            if w == s:
                line = line + ahalo15[s, 0:V]
            total = e15[s, w, 0] * line[0:1]
            for v in range(1, V):
                total = total + e15[s, w, v] * line[v : v + 1]
            gs15[s, w] = total
            for v in range(V):
                adj[v, s * (rows - 2) + w, ch - 1 : ch, :] = line[v : v + 1]
    for s in range(2):
        @pl.when(has[s])
        def _(s=s):
            single_copy(gs15, gr15, g15_s, g15_r, s).start()
    pair = 2 if members % 2 == 0 else 1

    def inside(b, carry):
        ks = [b * pair + g for g in range(pair)]
        parts = []
        for k in ks:
            total = ens[k, 0].astype(F32) * adj[0]
            for v in range(1, V):
                total = total + ens[k, v].astype(F32) * adj[v]
            parts.append(total.reshape(size, levels))
        hi, lo = split2(jnp.concatenate(parts, axis=1))
        hi, lo = split2(dot(mm[...], hi) + dot(mm[...], lo))
        for g, k in enumerate(ks):
            part = slice(g * levels, (g + 1) * levels)
            both = jnp.concatenate([hi[:, part], lo[:, part]], axis=1)
            out[k] = av[k].astype(F32) + dot(both, lv_nn).reshape(rows, cols, levels)
        return carry

    steps = members // pair
    stops = [0, steps // 5, 2 * steps // 5, steps]
    lax.fori_loop(stops[0], stops[1], inside, 0)
    for c in order[:2]:
        second.forward(2, c)
    lax.fori_loop(stops[1], stops[2], inside, 0)
    for c in order[2:]:
        second.forward(2, c)
    lax.fori_loop(stops[2], stops[3], inside, 0)
    for c in order:
        second.forward(3, c)

    for s in range(2):
        @pl.when(has[s])
        def _(s=s):
            remote(gr15.at[s], gr15.at[s], g15_s.at[s], g15_r.at[s], m, near[s]).wait_recv()
    for g in range(3):
        for c in order:
            second.receive(g, c)

    def outer(k):
        sides = []
        for s in range(2):
            turn_rows = (0, 1) if s == 0 else (1, 0)
            body = jnp.stack([jnp.concatenate([gr[o, s, k], gr[2 + o, s, k]], axis=0) for o in turn_rows])
            at = lax.broadcasted_iota(jnp.int32, body.shape, 1)
            line = jnp.stack([gr15[s, w, k : k + 1] for w in range(2)])
            sides.append(jnp.where(at == ch - 1, jnp.broadcast_to(line, body.shape), body))
        around = jnp.concatenate(sides, axis=0).reshape(4 * cols, levels)
        back = dot(em[...], jnp.concatenate(split2(around), axis=0))
        both = jnp.concatenate(split2(back), axis=1)
        add = dot(both, lv_nn).reshape(4, cols, levels)
        out[k, 0:2] += add[0:2]
        out[k, rows - 2 : rows] += add[2:4]

    for c in order:
        second.receive(3, c)
        for k in range(c * per, (c + 1) * per):
            outer(k)

    first.drain()
    second.drain()
    for g in range(3):
        to_mate(g).wait_send()
        for d in range(1, n // 2):
            to_peer(g, d).wait_send()
        back_to_mate(g).wait_send()
    for h in range(2):
        for s in range(2):
            @pl.when(has[s] & (p == s))
            def _(h=h, s=s):
                for d in range(n // 2):
                    outer_copy(h, s, d).wait_send()

            @pl.when(has[s])
            def _(h=h, s=s):
                near_copy(adjs, ahalo, ah_s, ah_r, h, s).wait_send()
    for s in range(2):
        @pl.when(has[s])
        def _(s=s):
            single_copy(adjs15, ahalo15, a15_s, a15_r, s).wait_send()
            single_copy(gs15, gr15, g15_s, g15_r, s).wait_send()


def solution(mesh):
    n = mesh.shape["mem"]
    tiles = mesh.shape["tile"]

    def on_device(alpha, ensemble, loc_vert, obs_col, obs_lev, obs_count, innovation, obs_weight):
        members, rows, cols, levels = alpha.shape
        slots = obs_col.shape[1]
        chunks = 4 if members % 4 == 0 else 1
        ch = cols // 2
        mid = (rows - 4) // 2
        vmem = pl.BlockSpec(memory_space=pltpu.VMEM)
        hbm = pl.BlockSpec(memory_space=pltpu.HBM)
        turned = pltpu.VMEM((2, 2, members, 2, ch, levels), F32)
        passing = pltpu.VMEM((2, members, 2, ch, levels), F32)
        line2 = pltpu.VMEM((4, 2, members, ch, levels), F32)
        passing2 = pltpu.VMEM((4, members, ch, levels), F32)
        dma = pltpu.SemaphoreType.DMA
        line = pltpu.VMEM((1, slots), F32)
        mark = pltpu.VMEM((1, slots), jnp.int32)
        padded = -(-members // 8) * 8
        thin = -(-6 * V // 16) * 16

        def sums(piece, result):
            return [pltpu.VMEM((2,) + piece, F32), pltpu.VMEM(piece, F32),
                    pltpu.VMEM((max(n // 2 - 1, 1),) + piece, F32), pltpu.VMEM((2,) + result, F32)]

        borders = pltpu.VMEM((2, 2, V, ch, levels), F32)
        small = pltpu.VMEM((2, 8, levels), F32)
        slim = pltpu.VMEM((2, 2, padded, levels), F32)
        return pl.pallas_call(
            functools.partial(kernel, n, tiles, chunks),
            out_shape=jax.ShapeDtypeStruct(alpha.shape, F32),
            in_specs=[hbm, hbm, hbm, hbm, hbm, pl.BlockSpec(memory_space=pltpu.SMEM), hbm, hbm],
            out_specs=vmem,
            scratch_shapes=[
                pltpu.VMEM(alpha.shape, BF16), pltpu.VMEM(ensemble.shape, BF16),
                pltpu.VMEM(loc_vert.shape, BF16), mark, mark, line, line,
                turned, turned, passing, line2, line2, passing2,
                pltpu.VMEM((rows * cols, rows * cols), BF16),
                pltpu.VMEM((4 * cols, 4 * cols), BF16),
                pltpu.VMEM((4 * cols, 8 * cols), BF16),
                pltpu.VMEM((2, thin + V * (rows + 2) * ch, slots), BF16),
                pltpu.VMEM((thin, slots), F32),
                pltpu.VMEM((2 * levels, slots), BF16),
                pltpu.VMEM((2, 2, V, padded, levels), F32),
                *sums((V, mid, cols, levels), (V, mid, cols, levels)),
                *sums((V, 2, ch, levels), (V, 3, ch, levels)), *sums((V, 2, ch, levels), (V, 3, ch, levels)),
                pltpu.VMEM((2, n // 2, V, ch, levels), F32), pltpu.VMEM((V, rows, cols, levels), F32), borders, borders,
                small, small, slim, slim,
                dma((9,)),
                dma((2, 2, chunks)), dma((2, 2, chunks)), dma((2, chunks)), dma((2, chunks)),
                dma((4, 2, chunks)), dma((4, 2, chunks)), dma((4, chunks)), dma((4, chunks)),
                dma((3, n // 2 + 1)), dma((3, n // 2 + 1)),
                dma((2, n // 2)), dma((2, n // 2)), dma((2, 2)), dma((2, 2)),
                dma((2,)), dma((2,)), dma((2,)), dma((2,)),
            ],
            compiler_params=pltpu.CompilerParams(
                collective_id=0, has_side_effects=True, vmem_limit_bytes=48 << 20),
        )(*[pltpu.with_memory_space_constraint(x, pltpu.HBM) for x in (alpha, ensemble, loc_vert, obs_col, obs_lev)],
          obs_count, *[pltpu.with_memory_space_constraint(x, pltpu.HBM) for x in (innovation, obs_weight)])

    in_specs = (
        P("mem", "tile", None, None),
        P("mem", None, "tile", None, None),
        P(),
        P("tile", None),
        P("tile", None),
        P("tile"),
        P("tile", None),
        P("tile", None),
    )
    out_specs = P("mem", "tile", None, None)
    return jax.shard_map(
        on_device, mesh=mesh, in_specs=in_specs, out_specs=out_specs, check_vma=False
    )
```

```python
import functools

import jax
import jax.numpy as jnp
from jax import lax
from jax.experimental import pallas as pl
from jax.experimental.pallas import tpu as pltpu
from jax.sharding import PartitionSpec as P

V = 3
F32 = jnp.float32
BF16 = jnp.bfloat16
MESH = pl.DeviceIdType.MESH


def split2(x):
    hi = x.astype(BF16)
    lo = (x - hi.astype(F32)).astype(BF16)
    return hi, lo


def dot(a, b):
    return jnp.dot(a, b, preferred_element_type=F32)


def dot_nt(a, b):
    return lax.dot_general(a, b, (((1,), (1,)), ((), ())), preferred_element_type=F32)


def band(distance):
    d = jnp.abs(distance)
    return jnp.where(d == 0, 6.0, jnp.where(d == 1, 4.0, jnp.where(d == 2, 1.0, 0.0)))


def column_weight(c, c2, cols):
    end = (c == c2) & ((c == 0) | (c == cols - 1))
    return (band(c - c2) - jnp.where(end, 1.0, 0.0)) * (1.0 / 16.0)


def kernel(n, tiles, chunks, alpha_h, ens_h, loc_h, col_h, lev_h, cnt, innov_h, wgt_h, out,
           av, ens, loc, col, lev, innov, wgt,
           hs, hr, hl, gs, gr, gl, mm, sc, em, wt, w15, sent, e15,
           bi, bi1, bi2, fi, b0, b01, b02, f0, b1, b11, b12, f1,
           iy, adj, adjs, ahalo, adjs15, ahalo15, gs15, gr15,
           in_sem, hs_s, hs_r, hl_s, hl_r, gs_s, gs_r, ge_r, gl_s, gl_r,
           sh_s, sh_r, ih_s, ih_r, ah_s, ah_r, ah_f, a15_s, a15_r, g15_s, g15_r):
    members, rows, cols, levels = out.shape
    size = rows * cols
    ch = cols // 2
    mid = (rows - 4) // 2
    per = members // chunks
    group = 4 if members % 4 == 0 else 1
    slots = col.shape[1]
    m = lax.axis_index("mem")
    t = lax.axis_index("tile")
    p = lax.rem(m, 2)
    mate = m + 1 - 2 * p
    has = (t > 0, t < tiles - 1)
    near = (t - 1, t + 1)
    edge = (slice(0, 2), slice(rows - 2, rows))
    half = (slice(0, ch), slice(ch, cols))

    def loads():
        pairs = (
            (alpha_h.at[:, 0:2], av.at[:, 0:2]),
            (alpha_h.at[:, rows - 2 : rows], av.at[:, rows - 2 : rows]),
            (loc_h, loc),
            (alpha_h.at[:, 2 : rows - 2], av.at[:, 2 : rows - 2]),
            (ens_h, ens),
            (col_h, col), (lev_h, lev), (innov_h, innov), (wgt_h, wgt))
        return [pltpu.make_async_copy(a, b, in_sem.at[i]) for i, (a, b) in enumerate(pairs)]

    copies = loads()
    for copy in copies:
        copy.start()

    relays = tiles % 2 == 0 and tiles >= 4
    lead = chunks // 2
    odd = lax.rem(t, 2)
    turn = tiles // 2
    share_out = lax.div(chunks * lax.div(t + odd, 2), max(turn, 1))
    n_out = odd * (chunks - share_out) + (1 - odd) * share_out
    share_in = lax.div(chunks * lax.div(t + 2 - 3 * odd, 2), max(turn, 1))
    n_in = (1 - odd) * (chunks - share_in) + odd * share_in
    far = (t >= 2, t <= tiles - 3)
    passes = jnp.where(odd == 1, t - 2, tiles - 3 - t) >= 0

    barrier = pltpu.get_barrier_semaphore()

    def greet(who, where):
        pl.semaphore_signal(barrier, inc=1, device_id={"mem": who, "tile": where}, device_id_type=MESH)

    for d in range(1, n):
        greet(lax.rem(m + d, n), t)
    total = jnp.int32(n - 1)
    for s in range(2):
        @pl.when(has[s])
        def _(s=s):
            for d in range(n // 2):
                greet(lax.rem(m + 2 * d, n), near[s])
        total = total + (n // 2) * has[s].astype(jnp.int32)
        if relays:
            @pl.when(far[s])
            def _(s=s):
                greet(m, t - 2 + 4 * s)
            total = total + far[s].astype(jnp.int32)

    def remote(src, dst, ssem, rsem, who, where):
        return pltpu.make_async_remote_copy(
            src_ref=src, dst_ref=dst, send_sem=ssem, recv_sem=rsem,
            device_id={"mem": who, "tile": where}, device_id_type=MESH)

    class Halo:
        def __init__(self, src, dst, via, ss, sr, vs, vr, groups, fine=None):
            self.src, self.dst, self.via = src, dst, via
            self.ss, self.sr, self.vs, self.vr = ss, sr, vs, vr
            self.groups, self.fine = groups, fine

        def group(self, h):
            return [b for b, span in enumerate(self.groups) if span[0] <= h < span[1]][0]

        def landed(self, h, s, c):
            if self.fine is not None and h == self.src.shape[0] - 1:
                return self.fine.at[s, c]
            return self.sr.at[self.group(h), s]

        def direct(self, h, s, c):
            part = pl.ds(c * per, per)
            return remote(self.src.at[h, s, part], self.dst.at[h, 1 - s, part],
                          self.ss.at[s], self.landed(h, 1 - s, c), m, near[s])

        def receive_chunk(self, h, c):
            for s in range(2):
                @pl.when(has[s])
                def _(s=s):
                    part = self.dst.at[h, s, pl.ds(c * per, per)]
                    remote(part, part, self.ss.at[s], self.landed(h, s, c), m, near[s]).wait_recv()

        def detour(self, h, s, c):
            part = pl.ds(c * per, per)
            return remote(self.src.at[h, s, part], self.via.at[h, part],
                          self.ss.at[s], self.vr.at[h, c], m, t + 1 - 2 * odd)

        def onward(self, h, c):
            part = pl.ds(c * per, per)
            return remote(self.via.at[h, part], self.dst.at[h, odd, part],
                          self.vs.at[0], self.landed(h, odd, c), m, t + 2 - 4 * odd)

        def send_turned(self, h, c):
            for s in range(2):
                if relays:
                    @pl.when(has[s] & (odd == s) & (c >= chunks - n_out))
                    def _(s=s):
                        self.detour(h, s, c).start()

        def send_far(self, h, c):
            for s in range(2):
                straight = c < chunks - n_out if relays else True

                @pl.when(has[s] & (odd == s) & straight)
                def _(s=s):
                    self.direct(h, s, c).start()

        def send_near(self, h, c, when=True):
            for s in range(2):
                @pl.when(has[s] & (odd != s) & when)
                def _(s=s):
                    self.direct(h, s, c).start()

        def send_close(self, h):
            for c in order:
                self.send_turned(h, c)
            for c in order:
                self.send_near(h, c)

        def forward(self, h, c):
            if relays:
                @pl.when(passes & (c >= chunks - n_in))
                def _():
                    self.onward_recv(h, c).wait_recv()
                    self.onward(h, c).start()

        def onward_recv(self, h, c):
            part = pl.ds(c * per, per)
            return remote(self.via.at[h, part], self.via.at[h, part],
                          self.vs.at[0], self.vr.at[h, c], m, t + 1 - 2 * odd)

        def receive(self, b):
            span = self.groups[b]
            for s in range(2):
                @pl.when(has[s])
                def _(s=s):
                    every = self.dst.at[span[0] : span[1], s]
                    remote(every, every, self.ss.at[s], self.sr.at[b, s], m, near[s]).wait_recv()

        def drain(self):
            for s in range(2):
                @pl.when(has[s])
                def _(s=s):
                    remote(self.src.at[:, s], self.dst.at[:, s], self.ss.at[s], self.sr.at[0, s], m, near[s]).wait_send()
            if relays:
                for count in range(1, chunks + 1):
                    @pl.when(passes & (n_in == count))
                    def _(count=count):
                        every = self.via.at[:, members - count * per : members]
                        remote(every, every, self.vs.at[0], self.sr.at[0, 0], m, t + 2 - 4 * odd).wait_send()

    first = Halo(hs, hr, hl, hs_s, hs_r, hl_s, hl_r, ((0, 1), (1, 2)))
    second = Halo(gs, gr, gl, gs_s, gs_r, gl_s, gl_r, ((0, 3),), ge_r)
    order = list(range(chunks - 1, -1, -1))

    i = lax.broadcasted_iota(jnp.int32, (4 * cols, 4 * cols), 0)
    j = lax.broadcasted_iota(jnp.int32, (4 * cols, 4 * cols), 1)
    q, q2 = lax.div(i, cols), lax.div(j, cols)
    across = column_weight(i - q * cols, j - q2 * cols, cols)
    sc[...] = (jnp.where(q == q2, 1.0 / 16.0, 0.0) * across).astype(BF16)
    r = jnp.where(q < 2, q, q + rows - 4)
    r2 = jnp.where(q2 < 2, q2 - 2, q2 - 2 + rows)
    corner = (band(r - r2) * (1.0 / 16.0) * across).astype(BF16)
    em[:, 0 : 4 * cols] = corner
    em[:, 4 * cols :] = corner

    for k in range(3):
        copies[k].wait()
    lv = loc[...]
    lv_nt = jnp.concatenate([lv, lv], axis=1)
    lv_nn = jnp.concatenate([lv, lv], axis=0)

    def prepare(k):
        x = jnp.concatenate([av[k, 0:2], av[k, rows - 2 : rows]], axis=0).reshape(4 * cols, levels)
        both = jnp.concatenate(split2(dot(sc[...], x)), axis=1)
        u = dot_nt(both, lv_nt).reshape(4, cols, levels)
        for s in range(2):
            for h in range(2):
                hs[h, s, k] = u[2 * s : 2 * s + 2, half[h]]

    for c in order:
        for k in range(c * per, (c + 1) * per):
            prepare(k)
        if c == order[0]:
            pl.semaphore_wait(barrier, total)
        first.send_turned(0, c)
        first.send_far(0, c)
        if c != order[0]:
            first.send_near(0, c + 1)
    first.send_near(0, order[-1])
    for c in order:
        first.send_turned(1, c)
    ahead = [(chunks - c) + n_out <= lead for c in range(chunks)]
    for c in order:
        first.send_near(1, c, ahead[c])
    for s in range(2):
        @pl.when(jnp.logical_not(has[s]))
        def _(s=s):
            for ref in (hr, gr, ahalo):
                for h in range(ref.shape[0]):
                    ref[h, s] = jnp.zeros(ref.shape[2:], F32)
            ahalo15[s] = jnp.zeros(ahalo15.shape[1:], F32)
            gr15[s] = jnp.zeros(gr15.shape[1:], F32)

    i = lax.broadcasted_iota(jnp.int32, (size, size), 0)
    j = lax.broadcasted_iota(jnp.int32, (size, size), 1)
    r, r2 = lax.div(i, cols), lax.div(j, cols)
    end = (r == r2) & (((r == 0) & (t == 0)) | ((r == rows - 1) & (t == tiles - 1)))
    row_weight = (band(r - r2) - jnp.where(end, 1.0, 0.0)) * (1.0 / 16.0)
    mm[...] = (row_weight * column_weight(i - r * cols, j - r2 * cols, cols)).astype(BF16)

    stage_refs = ((b0, b01, b02, f0), (b1, b11, b12, f1), (bi, bi1, bi2, fi))
    for ref in (b0, b1, bi):
        ref[...] = jnp.zeros_like(ref)
    copies[3].wait()
    copies[4].wait()

    def lift(b, carry):
        ks = [b * group + g for g in range(group)]
        x = jnp.concatenate([av[k].reshape(size, levels) for k in ks], axis=1)
        hi, lo = split2(dot(mm[...], x))
        bases = []
        for g in range(group):
            part = slice(g * levels, (g + 1) * levels)
            both = jnp.concatenate([hi[:, part], lo[:, part]], axis=1)
            bases.append(dot_nt(both, lv_nt).reshape(rows, cols, levels))
        for v in range(V):
            total = ens[ks[0], v].astype(F32) * bases[0]
            for g in range(1, group):
                total = total + ens[ks[g], v].astype(F32) * bases[g]
            for s in range(2):
                bi[s, v] += total[2 + s * mid : 2 + (s + 1) * mid]
                b0[s, v] += total[edge[s], half[0]]
                b1[s, v] += total[edge[s], half[1]]
        return carry

    lax.fori_loop(0, members // group, lift, 0)

    def to_mate(g):
        part, rec, rec2, full = stage_refs[g]
        return remote(part.at[1 - p], rec, sh_s.at[g, 0], sh_r.at[g, 0], mate, t)

    def to_peer(g, d):
        part, rec, rec2, full = stage_refs[g]
        return remote(part.at[p], rec2.at[d - 1], sh_s.at[g, d], sh_r.at[g, d], lax.rem(m + 2 * d, n), t)

    def back_to_mate(g):
        part, rec, rec2, full = stage_refs[g]
        return remote(full.at[p], full.at[p], sh_s.at[g, n // 2], sh_r.at[g, n // 2], mate, t)

    def back_from_mate(g):
        part, rec, rec2, full = stage_refs[g]
        return remote(full.at[1 - p], full.at[1 - p], sh_s.at[g, n // 2], sh_r.at[g, n // 2], mate, t)

    def reduce_chip(g):
        part, rec, rec2, full = stage_refs[g]
        to_mate(g).wait_recv()
        part[p] += rec[...]
        for d in range(1, n // 2):
            to_peer(g, d).start()

    def reduce_rest(g):
        part, rec, rec2, full = stage_refs[g]
        total = part[p]
        for d in range(1, n // 2):
            to_peer(g, d).wait_recv()
            total = total + rec2[d - 1]
        return total

    def outer_copy(h, s, d):
        here = lax.div(m, 2)
        return remote(stage_refs[h][0].at[p, :, s], iy.at[h, here], ih_s.at[h, d], ih_r.at[h, here],
                      lax.rem(m + 2 * d, n), near[s])

    def outer_send(h):
        for s in range(2):
            @pl.when(has[s] & (p == s))
            def _(s=s):
                for d in range(n // 2):
                    outer_copy(h, s, d).start()

    def outer_recv(h):
        full = stage_refs[h][3]
        for s in range(2):
            @pl.when(has[1 - s] & (p == s))
            def _(s=s):
                total = None
                for d in range(n // 2):
                    remote(iy.at[h, d], iy.at[h, d], ih_s.at[h, 0], ih_r.at[h, d], m, near[1 - s]).wait_recv()
                    total = iy[h, d] if total is None else total + iy[h, d]
                full[s, :, 2] = total

            @pl.when(jnp.logical_not(has[1 - s]) & (p == s))
            def _(s=s):
                full[s, :, 2] = jnp.zeros(full.shape[1:2] + full.shape[3:], F32)

    to_mate(2).start()
    first.forward(0, order[0])
    for k in range(5, 9):
        copies[k].wait()

    place = col[...]
    wide = 2 * cols
    frow = lax.div(place, wide)
    fcol = place - frow * wide
    slot = lax.broadcasted_iota(jnp.int32, (1, slots), 1)
    variable = lax.rem(slot, V)
    early = fcol <= 2 * (ch - 1)
    live = slot < cnt[0]

    def weights(fine, count, shift):
        main = lax.div(fine, 2)
        other = jnp.where(fine - 2 * main == 1, main + 1, main - 1)
        at = lax.broadcasted_iota(jnp.int32, (count, slots), 0) - shift
        return jnp.where(at == main, 0.75, 0.0) + jnp.where(at == other, 0.25, 0.0)

    wr = weights(frow, rows + 2, 1)
    wc = weights(fcol, cols, 0)
    head = w15.shape[0]
    w15[...] = jnp.zeros_like(w15)
    rim = [0, 1, 2, rows - 1, rows, rows + 1]
    lines = rim + list(range(3, rows - 1))
    cut = head + len(rim) * V * ch
    for v in range(V):
        mask = jnp.where(variable == v, 1.0, 0.0)
        for b, a in enumerate(lines):
            start = head + (b * V + v) * ch
            line = wr[a : a + 1, :] * mask
            for h in range(2):
                wt[h, start : start + ch, :] = (wc[half[h]] * line).astype(BF16)
            if b < len(rim):
                w15[b * V + v : b * V + v + 1, :] = wc[ch - 1 : ch] * line
        if v == 0:
            reduce_chip(2)
    wt[1, 0:head, :] = w15[...].astype(BF16)
    for c in order[1:2]:
        first.forward(0, c)
    fi[p] = reduce_rest(2)
    back_to_mate(2).start()

    e15[...] = jnp.zeros_like(e15)
    for s in range(2):
        for w in range(2):
            row = s * (rows - 2) + w
            for v in range(V):
                for k in range(members):
                    e15[s, w, v, k : k + 1, :] = ens[k, v, row, ch - 1 : ch, :].astype(F32)

    def edge_increment(h, c):
        part = stage_refs[h][0]
        sums = [[None] * V for _ in range(2)]
        for k in range(c * per, (c + 1) * per):
            above, below = hr[h, 0, k], hr[h, 1, k]
            fields = (jnp.stack([above[0] + 4.0 * above[1], above[1]]),
                      jnp.stack([below[0], 4.0 * below[0] + below[1]]))
            for s in range(2):
                for v in range(V):
                    term = ens[k, v, edge[s], half[h]].astype(F32) * fields[s]
                    sums[s][v] = term if sums[s][v] is None else sums[s][v] + term
        for s in range(2):
            for v in range(V):
                part[s, v] += sums[s][v]

    hot = lax.broadcasted_iota(jnp.int32, (levels, slots), 0) == lev[...]

    def pick(h, pieces, start):
        flat = jnp.concatenate(pieces, axis=0).reshape(-1, levels)
        both = jnp.concatenate(split2(flat.T), axis=0)
        picked = dot(both, wt[h, start : start + flat.shape[0]])
        return jnp.sum(jnp.where(hot, picked[:levels] + picked[levels:], 0.0), axis=0, keepdims=True)

    def pick_inner(h):
        return pick(h, [fi[s, :, a, half[h]] for s in range(2) for a in range(mid)], cut)

    def pick_rim(h):
        full = stage_refs[h][3]
        return pick(h, [full[1, :, 2], full[0, :, 0], full[0, :, 1], full[1, :, 0], full[1, :, 1], full[0, :, 2]], head)

    def spread(weighted):
        hi, lo = split2(jnp.where(hot, jnp.broadcast_to(weighted, hot.shape), 0.0))
        sent[0:levels, :] = hi
        sent[levels:, :] = lo

    def adjoint(h, start, stop):
        both = dot_nt(wt[h, start:stop, :], sent[...])
        return both[:, :levels] + both[:, levels:]

    def shaped(x):
        return x.reshape(x.shape[0] // (V * ch), V, ch, levels)

    def edge_copy(h, s):
        return remote(adjs.at[h, s], ahalo.at[h, 1 - s], ah_s.at[h], ah_r.at[h, 1 - s], m, near[s])

    def hand_over(h, s):
        return remote(ahalo.at[h, s], ahalo.at[h, s], ah_f.at[h], ah_r.at[h, s], mate, t)

    def single_copy(src, dst, ssem, rsem, s):
        return remote(src.at[s], dst.at[1 - s], ssem.at[s], rsem.at[1 - s], m, near[s])

    def adjoint_edges(h):
        flat = adjoint(h, head * (1 - h), cut)
        thin = flat[:head] if h else None
        rims = shaped(flat[head * h :])
        adjs[h, 0] = rims[0]
        adjs[h, 1] = rims[5]
        if h:
            adjs15[0, 0:V] = thin[0:V]
            adjs15[1, 0:V] = thin[5 * V : 6 * V]
        for s in range(2):
            @pl.when(has[s] & (p == s))
            def _(s=s):
                edge_copy(h, s).start()

            @pl.when(has[s])
            def _(s=s):
                if h:
                    single_copy(adjs15, ahalo15, a15_s, a15_r, s).start()
        for a in range(2):
            adj[:, a, half[h]] = rims[1 + a]
            adj[:, rows - 2 + a, half[h]] = rims[3 + a]
        return thin

    def adjoint_halo(h):
        for s in range(2):
            @pl.when(has[s] & (p == 1 - s))
            def _(s=s):
                hand_over(h, s).wait_recv()
                hand_over(h, s).start()
        for s in range(2):
            @pl.when(has[s] & (p == s))
            def _(s=s):
                hand_over(h, s).wait_recv()
        adj[:, 0, half[h]] += ahalo[h, 0]
        adj[:, rows - 1, half[h]] += ahalo[h, 1]

    def fields(h, outermost):
        where = (0, rows - 1) if outermost else (1, rows - 2)
        weights = [[adj[v, where[s], half[h]] for v in range(V)] for s in range(2)]
        for k in range(members):
            for s in range(2):
                total = ens[k, 0, where[s], half[h]].astype(F32) * weights[s][0]
                for v in range(1, V):
                    total = total + ens[k, v, where[s], half[h]].astype(F32) * weights[s][v]
                gs[2 * h + outermost, s, k] = total

    def chain_open(h):
        first.receive(h)
        for c in order:
            edge_increment(h, c)
        to_mate(h).start()
        reduce_chip(h)
        outer_send(h)

    def chain_close(h, between, after):
        full = stage_refs[h][3]
        full[p, :, 0:2] = reduce_rest(h)
        between()
        outer_recv(h)
        back_to_mate(h).start()
        after()
        back_from_mate(h).wait_recv()

    back_from_mate(2).wait_recv()
    value = pick_inner(0)
    for c in order[2:]:
        first.forward(0, c)
    value = value + pick_inner(1)

    def release(halo, h):
        for c in order:
            halo.send_far(h, c)

    def between_a():
        release(first, 1)
        first.forward(1, order[0])

    chain_open(0)
    for c in order:
        first.send_near(1, c, jnp.logical_not(ahead[c]))
    chain_close(0, between_a, lambda: None)
    for c in order[1:2]:
        first.forward(1, c)
    value = value + pick_rim(0)
    weighted = jnp.where(live & early, wgt[...] * (value - innov[...]), 0.0)
    spread(weighted)
    adjoint_edges(0)
    fields(0, 0)
    for c in order:
        second.send_turned(0, c)
    for c in order:
        second.send_near(0, c, ahead[c])
    for c in order[2:]:
        first.forward(1, c)

    chain_open(1)
    for c in order:
        second.send_near(0, c, jnp.logical_not(ahead[c]))
    adjoint_halo(0)
    fields(0, 1)
    second.send_close(1)
    for c in order[:2]:
        second.forward(0, c)
    chain_close(1, lambda: release(second, 0), lambda: release(second, 1))
    for c in order[2:]:
        second.forward(0, c)
    value = value + pick_rim(1)
    spread(jnp.where(live, wgt[...] * (value - innov[...]), 0.0))
    thin = adjoint_edges(1)
    fields(1, 0)
    second.send_close(2)
    for c in order:
        second.forward(1, c)
    for h in range(2):
        inner = shaped(adjoint(h, cut, wt.shape[1]))
        for a in range(rows - 4):
            adj[:, 2 + a, half[h]] = inner[a]
    adjoint_halo(1)
    for s in range(2):
        @pl.when(has[s])
        def _(s=s):
            remote(ahalo15.at[s], ahalo15.at[s], a15_s.at[s], a15_r.at[s], m, near[s]).wait_recv()
    for s in range(2):
        for w in range(2):
            a = 1 + 2 * s + w
            line = thin[a * V : (a + 1) * V]
            if w == s:
                line = line + ahalo15[s, 0:V]
            total = e15[s, w, 0] * line[0:1]
            for v in range(1, V):
                total = total + e15[s, w, v] * line[v : v + 1]
            gs15[s, w] = total
            for v in range(V):
                adj[v, s * (rows - 2) + w, ch - 1 : ch, :] = line[v : v + 1]
    for s in range(2):
        @pl.when(has[s])
        def _(s=s):
            single_copy(gs15, gr15, g15_s, g15_r, s).start()
    fields(1, 1)
    for c in order:
        second.send_far(2, c)
    second.send_close(3)
    for c in order:
        second.send_far(3, c)

    pair = group

    def inside(b, carry):
        ks = [b * pair + g for g in range(pair)]
        parts = []
        for k in ks:
            total = ens[k, 0].astype(F32) * adj[0]
            for v in range(1, V):
                total = total + ens[k, v].astype(F32) * adj[v]
            parts.append(total.reshape(size, levels))
        hi, lo = split2(jnp.concatenate(parts, axis=1))
        hi, lo = split2(dot(mm[...], hi) + dot(mm[...], lo))
        for g, k in enumerate(ks):
            part = slice(g * levels, (g + 1) * levels)
            both = jnp.concatenate([hi[:, part], lo[:, part]], axis=1)
            out[k] = av[k].astype(F32) + dot(both, lv_nn).reshape(rows, cols, levels)
        return carry

    steps = members // pair
    stops = [0, steps // 5, 2 * steps // 5, steps]
    lax.fori_loop(stops[0], stops[1], inside, 0)
    for c in order[:2]:
        second.forward(2, c)
    lax.fori_loop(stops[1], stops[2], inside, 0)
    for c in order[2:]:
        second.forward(2, c)
    lax.fori_loop(stops[2], stops[3], inside, 0)

    def outer_early(b, carry):
        ks = [b * pair + g for g in range(pair)]
        parts = []
        for k in ks:
            sides = []
            for s in range(2):
                for o in ((0, 1) if s == 0 else (1, 0)):
                    at = lax.broadcasted_iota(jnp.int32, (ch, levels), 0)
                    sides.append(jnp.where(at == ch - 1, 0.0, gr[o, s, k]))
                    sides.append(gr[2, s, k] if o == 0 else jnp.zeros((ch, levels), F32))
            parts.append(jnp.concatenate(sides, axis=0))
        back = dot(em[...], jnp.concatenate(split2(jnp.concatenate(parts, axis=1)), axis=0))
        hi, lo = split2(back)
        for g, k in enumerate(ks):
            part = slice(g * levels, (g + 1) * levels)
            both = jnp.concatenate([hi[:, part], lo[:, part]], axis=1)
            add = dot(both, lv_nn).reshape(4, cols, levels)
            out[k, 0:2] += add[0:2]
            out[k, rows - 2 : rows] += add[2:4]
        return carry

    for c in order[:1]:
        second.forward(3, c)
    second.receive(0)
    third = steps // 3
    lax.fori_loop(0, third, outer_early, 0)
    for c in order[1:2]:
        second.forward(3, c)
    lax.fori_loop(third, 2 * third, outer_early, 0)
    for c in order[2:]:
        second.forward(3, c)
    lax.fori_loop(2 * third, steps, outer_early, 0)

    i = lax.broadcasted_iota(jnp.int32, (4 * cols, 2 * ch + 16), 0)
    j = lax.broadcasted_iota(jnp.int32, (4 * cols, 2 * ch + 16), 1)
    q = lax.div(i, cols)
    r = jnp.where(q < 2, q, q + rows - 4)
    spot = j - 2 * ch
    r2 = jnp.where(spot < 0, jnp.where(j < ch, -1, rows), jnp.where(spot < 2, spot - 2, spot - 2 + rows))
    c2 = jnp.where(spot < 0, jnp.where(j < ch, j, j - ch) + ch, ch - 1)
    last = band(r - r2) * (1.0 / 16.0) * column_weight(i - q * cols, c2, cols)
    last = jnp.where(spot < 4, last, 0.0).astype(BF16)
    last = jnp.concatenate([last, last], axis=1)

    for s in range(2):
        @pl.when(has[s])
        def _(s=s):
            remote(gr15.at[s], gr15.at[s], g15_s.at[s], g15_r.at[s], m, near[s]).wait_recv()
    blank = jnp.zeros((12, levels), F32)

    def outer_late(c):
        ks = list(range(c * per, (c + 1) * per))
        rowsets = []
        for k in ks:
            rowsets += [gr[3, 0, k], gr[3, 1, k]] + [gr15[s, w, k : k + 1] for s in range(2) for w in range(2)] + [blank]
        both = jnp.concatenate(split2(jnp.concatenate(rowsets, axis=0)), axis=1)
        hi, lo = split2(dot(both, lv_nn))
        span = 2 * ch + 16
        stack = jnp.concatenate(
            [jnp.concatenate([x[g * span : (g + 1) * span] for g in range(len(ks))], axis=1) for x in (hi, lo)], axis=0)
        add = dot(last, stack)
        for g, k in enumerate(ks):
            piece = add[:, g * levels : (g + 1) * levels].reshape(4, cols, levels)
            out[k, 0:2] += piece[0:2]
            out[k, rows - 2 : rows] += piece[2:4]

    for c in order:
        second.receive_chunk(3, c)
        outer_late(c)

    first.drain()
    second.drain()
    for g in range(3):
        to_mate(g).wait_send()
        for d in range(1, n // 2):
            to_peer(g, d).wait_send()
        back_to_mate(g).wait_send()
    for h in range(2):
        for s in range(2):
            @pl.when(has[s] & (p == s))
            def _(h=h, s=s):
                for d in range(n // 2):
                    outer_copy(h, s, d).wait_send()

            @pl.when(has[s] & (p == s))
            def _(h=h, s=s):
                edge_copy(h, s).wait_send()

            @pl.when(has[s] & (p == 1 - s))
            def _(h=h, s=s):
                hand_over(h, s).wait_send()
    for s in range(2):
        @pl.when(has[s])
        def _(s=s):
            single_copy(adjs15, ahalo15, a15_s, a15_r, s).wait_send()
            single_copy(gs15, gr15, g15_s, g15_r, s).wait_send()


def solution(mesh):
    n = mesh.shape["mem"]
    tiles = mesh.shape["tile"]

    def on_device(alpha, ensemble, loc_vert, obs_col, obs_lev, obs_count, innovation, obs_weight):
        members, rows, cols, levels = alpha.shape
        slots = obs_col.shape[1]
        chunks = 4 if members % 4 == 0 else 1
        ch = cols // 2
        mid = (rows - 4) // 2
        vmem = pl.BlockSpec(memory_space=pltpu.VMEM)
        hbm = pl.BlockSpec(memory_space=pltpu.HBM)
        turned = pltpu.VMEM((2, 2, members, 2, ch, levels), F32)
        passing = pltpu.VMEM((2, members, 2, ch, levels), F32)
        line2 = pltpu.VMEM((4, 2, members, ch, levels), F32)
        passing2 = pltpu.VMEM((4, members, ch, levels), F32)
        dma = pltpu.SemaphoreType.DMA
        line = pltpu.VMEM((1, slots), F32)
        mark = pltpu.VMEM((1, slots), jnp.int32)
        padded = -(-members // 8) * 8
        thin = -(-6 * V // 16) * 16

        def sums(piece, result):
            return [pltpu.VMEM((2,) + piece, F32), pltpu.VMEM(piece, F32),
                    pltpu.VMEM((max(n // 2 - 1, 1),) + piece, F32), pltpu.VMEM((2,) + result, F32)]

        borders = pltpu.VMEM((2, 2, V, ch, levels), F32)
        small = pltpu.VMEM((2, 8, levels), F32)
        slim = pltpu.VMEM((2, 2, padded, levels), F32)
        return pl.pallas_call(
            functools.partial(kernel, n, tiles, chunks),
            out_shape=jax.ShapeDtypeStruct(alpha.shape, F32),
            in_specs=[hbm, hbm, hbm, hbm, hbm, pl.BlockSpec(memory_space=pltpu.SMEM), hbm, hbm],
            out_specs=vmem,
            scratch_shapes=[
                pltpu.VMEM(alpha.shape, BF16), pltpu.VMEM(ensemble.shape, BF16),
                pltpu.VMEM(loc_vert.shape, BF16), mark, mark, line, line,
                turned, turned, passing, line2, line2, passing2,
                pltpu.VMEM((rows * cols, rows * cols), BF16),
                pltpu.VMEM((4 * cols, 4 * cols), BF16),
                pltpu.VMEM((4 * cols, 8 * cols), BF16),
                pltpu.VMEM((2, thin + V * (rows + 2) * ch, slots), BF16),
                pltpu.VMEM((thin, slots), F32),
                pltpu.VMEM((2 * levels, slots), BF16),
                pltpu.VMEM((2, 2, V, padded, levels), F32),
                *sums((V, mid, cols, levels), (V, mid, cols, levels)),
                *sums((V, 2, ch, levels), (V, 3, ch, levels)), *sums((V, 2, ch, levels), (V, 3, ch, levels)),
                pltpu.VMEM((2, n // 2, V, ch, levels), F32), pltpu.VMEM((V, rows, cols, levels), F32), borders, borders,
                small, small, slim, slim,
                dma((9,)),
                dma((2,)), dma((2, 2)), dma((1,)), dma((2, chunks)),
                dma((2,)), dma((1, 2)), dma((2, chunks)), dma((1,)), dma((4, chunks)),
                dma((3, n // 2 + 1)), dma((3, n // 2 + 1)),
                dma((2, n // 2)), dma((2, n // 2)), dma((2,)), dma((2, 2)), dma((2,)),
                dma((2,)), dma((2,)), dma((2,)), dma((2,)),
            ],
            compiler_params=pltpu.CompilerParams(
                collective_id=0, has_side_effects=True, vmem_limit_bytes=48 << 20),
        )(*[pltpu.with_memory_space_constraint(x, pltpu.HBM) for x in (alpha, ensemble, loc_vert, obs_col, obs_lev)],
          obs_count, *[pltpu.with_memory_space_constraint(x, pltpu.HBM) for x in (innovation, obs_weight)])

    in_specs = (
        P("mem", "tile", None, None),
        P("mem", None, "tile", None, None),
        P(),
        P("tile", None),
        P("tile", None),
        P("tile"),
        P("tile", None),
        P("tile", None),
    )
    out_specs = P("mem", "tile", None, None)
    return jax.shard_map(
        on_device, mesh=mesh, in_specs=in_specs, out_specs=out_specs, check_vma=False
    )
```

```python
import functools

import jax
import jax.numpy as jnp
from jax import lax
from jax.experimental import pallas as pl
from jax.experimental.pallas import tpu as pltpu
from jax.sharding import PartitionSpec as P

V = 3
F32 = jnp.float32
BF16 = jnp.bfloat16
MESH = pl.DeviceIdType.MESH


def split2(x):
    hi = x.astype(BF16)
    lo = (x - hi.astype(F32)).astype(BF16)
    return hi, lo


def dot(a, b):
    return jnp.dot(a, b, preferred_element_type=F32)


def dot_nt(a, b):
    return lax.dot_general(a, b, (((1,), (1,)), ((), ())), preferred_element_type=F32)


def band(distance):
    d = jnp.abs(distance)
    return jnp.where(d == 0, 6.0, jnp.where(d == 1, 4.0, jnp.where(d == 2, 1.0, 0.0)))


def column_weight(c, c2, cols):
    end = (c == c2) & ((c == 0) | (c == cols - 1))
    return (band(c - c2) - jnp.where(end, 1.0, 0.0)) * (1.0 / 16.0)


def kernel(n, tiles, chunks, alpha_h, ens_h, loc_h, col_h, lev_h, cnt, innov_h, wgt_h, out,
           av, ens, loc, col, lev, innov, wgt,
           hs, hr, hl, gs, gr, gl, mm, sc, em, wt, w15, sent, e15,
           bi, bi1, bi2, fi, b0, b01, b02, f0, b1, b11, b12, f1,
           iy, adj, adjs, ahalo, adjs15, ahalo15, gs15, gr15,
           in_sem, hs_s, hs_r, hl_s, hl_r, gs_s, gs_r, ge_r, gl_s, gl_r,
           sh_s, sh_r, ih_s, ih_r, ah_s, ah_r, ah_f, a15_s, a15_r, g15_s, g15_r):
    members, rows, cols, levels = out.shape
    size = rows * cols
    ch = cols // 2
    mid = (rows - 4) // 2
    per = members // chunks
    group = 4 if members % 4 == 0 else 1
    slots = col.shape[1]
    m = lax.axis_index("mem")
    t = lax.axis_index("tile")
    p = lax.rem(m, 2)
    mate = m + 1 - 2 * p
    has = (t > 0, t < tiles - 1)
    near = (t - 1, t + 1)
    edge = (slice(0, 2), slice(rows - 2, rows))
    half = (slice(0, ch), slice(ch, cols))

    def loads():
        pairs = (
            (alpha_h.at[:, 0:2], av.at[:, 0:2]),
            (alpha_h.at[:, rows - 2 : rows], av.at[:, rows - 2 : rows]),
            (loc_h, loc),
            (alpha_h.at[:, 2 : rows - 2], av.at[:, 2 : rows - 2]),
            (ens_h, ens),
            (col_h, col), (lev_h, lev), (innov_h, innov), (wgt_h, wgt))
        return [pltpu.make_async_copy(a, b, in_sem.at[i]) for i, (a, b) in enumerate(pairs)]

    copies = loads()
    for copy in copies:
        copy.start()

    relays = tiles % 2 == 0 and tiles >= 4
    lead = chunks // 2
    odd = lax.rem(t, 2)
    turn = tiles // 2
    share_out = lax.div(chunks * lax.div(t + odd, 2), max(turn, 1))
    n_out = odd * (chunks - share_out) + (1 - odd) * share_out
    share_in = lax.div(chunks * lax.div(t + 2 - 3 * odd, 2), max(turn, 1))
    n_in = (1 - odd) * (chunks - share_in) + odd * share_in
    far = (t >= 2, t <= tiles - 3)
    passes = jnp.where(odd == 1, t - 2, tiles - 3 - t) >= 0

    barrier = pltpu.get_barrier_semaphore()

    def greet(who, where):
        pl.semaphore_signal(barrier, inc=1, device_id={"mem": who, "tile": where}, device_id_type=MESH)

    for d in range(1, n):
        greet(lax.rem(m + d, n), t)
    total = jnp.int32(n - 1)
    for s in range(2):
        @pl.when(has[s])
        def _(s=s):
            for d in range(n // 2):
                greet(lax.rem(m + 2 * d, n), near[s])
        total = total + (n // 2) * has[s].astype(jnp.int32)
        if relays:
            @pl.when(far[s])
            def _(s=s):
                greet(m, t - 2 + 4 * s)
            total = total + far[s].astype(jnp.int32)

    def remote(src, dst, ssem, rsem, who, where):
        return pltpu.make_async_remote_copy(
            src_ref=src, dst_ref=dst, send_sem=ssem, recv_sem=rsem,
            device_id={"mem": who, "tile": where}, device_id_type=MESH)

    class Halo:
        def __init__(self, src, dst, via, ss, sr, vs, vr, groups, fine=None):
            self.src, self.dst, self.via = src, dst, via
            self.ss, self.sr, self.vs, self.vr = ss, sr, vs, vr
            self.groups, self.fine = groups, fine

        def group(self, h):
            return [b for b, span in enumerate(self.groups) if span[0] <= h < span[1]][0]

        def landed(self, h, s, c):
            if self.fine is not None and h == self.src.shape[0] - 1:
                return self.fine.at[s, c]
            return self.sr.at[self.group(h), s]

        def direct(self, h, s, c):
            part = pl.ds(c * per, per)
            return remote(self.src.at[h, s, part], self.dst.at[h, 1 - s, part],
                          self.ss.at[s], self.landed(h, 1 - s, c), m, near[s])

        def receive_chunk(self, h, c):
            for s in range(2):
                @pl.when(has[s])
                def _(s=s):
                    part = self.dst.at[h, s, pl.ds(c * per, per)]
                    remote(part, part, self.ss.at[s], self.landed(h, s, c), m, near[s]).wait_recv()

        def detour(self, h, s, c):
            part = pl.ds(c * per, per)
            return remote(self.src.at[h, s, part], self.via.at[h, part],
                          self.ss.at[s], self.vr.at[h, c], m, t + 1 - 2 * odd)

        def onward(self, h, c):
            part = pl.ds(c * per, per)
            return remote(self.via.at[h, part], self.dst.at[h, odd, part],
                          self.vs.at[0], self.landed(h, odd, c), m, t + 2 - 4 * odd)

        def send_turned(self, h, c):
            for s in range(2):
                if relays:
                    @pl.when(has[s] & (odd == s) & (c >= chunks - n_out))
                    def _(s=s):
                        self.detour(h, s, c).start()

        def send_far(self, h, c):
            for s in range(2):
                straight = c < chunks - n_out if relays else True

                @pl.when(has[s] & (odd == s) & straight)
                def _(s=s):
                    self.direct(h, s, c).start()

        def send_near(self, h, c, when=True):
            for s in range(2):
                @pl.when(has[s] & (odd != s) & when)
                def _(s=s):
                    self.direct(h, s, c).start()

        def send_close(self, h):
            for c in order:
                self.send_turned(h, c)
            for c in order:
                self.send_near(h, c)

        def forward(self, h, c):
            if relays:
                @pl.when(passes & (c >= chunks - n_in))
                def _():
                    self.onward_recv(h, c).wait_recv()
                    self.onward(h, c).start()

        def onward_recv(self, h, c):
            part = pl.ds(c * per, per)
            return remote(self.via.at[h, part], self.via.at[h, part],
                          self.vs.at[0], self.vr.at[h, c], m, t + 1 - 2 * odd)

        def receive(self, b):
            span = self.groups[b]
            for s in range(2):
                @pl.when(has[s])
                def _(s=s):
                    every = self.dst.at[span[0] : span[1], s]
                    remote(every, every, self.ss.at[s], self.sr.at[b, s], m, near[s]).wait_recv()

        def drain(self):
            for s in range(2):
                @pl.when(has[s])
                def _(s=s):
                    remote(self.src.at[:, s], self.dst.at[:, s], self.ss.at[s], self.sr.at[0, s], m, near[s]).wait_send()
            if relays:
                for count in range(1, chunks + 1):
                    @pl.when(passes & (n_in == count))
                    def _(count=count):
                        every = self.via.at[:, members - count * per : members]
                        remote(every, every, self.vs.at[0], self.sr.at[0, 0], m, t + 2 - 4 * odd).wait_send()

    first = Halo(hs, hr, hl, hs_s, hs_r, hl_s, hl_r, ((0, 1), (1, 2)))
    second = Halo(gs, gr, gl, gs_s, gs_r, gl_s, gl_r, ((0, 3),), ge_r)
    order = list(range(chunks - 1, -1, -1))

    i = lax.broadcasted_iota(jnp.int32, (4 * cols, 4 * cols), 0)
    j = lax.broadcasted_iota(jnp.int32, (4 * cols, 4 * cols), 1)
    q, q2 = lax.div(i, cols), lax.div(j, cols)
    across = column_weight(i - q * cols, j - q2 * cols, cols)
    sc[...] = (jnp.where(q == q2, 1.0 / 16.0, 0.0) * across).astype(BF16)
    r = jnp.where(q < 2, q, q + rows - 4)
    r2 = jnp.where(q2 < 2, q2 - 2, q2 - 2 + rows)
    corner = (band(r - r2) * (1.0 / 16.0) * across).astype(BF16)
    em[:, 0 : 4 * cols] = corner
    em[:, 4 * cols :] = corner

    for k in range(3):
        copies[k].wait()
    lv = loc[...]
    lv_nt = jnp.concatenate([lv, lv], axis=1)
    lv_nn = jnp.concatenate([lv, lv], axis=0)

    def prepare(k):
        x = jnp.concatenate([av[k, 0:2], av[k, rows - 2 : rows]], axis=0).reshape(4 * cols, levels)
        both = jnp.concatenate(split2(dot(sc[...], x)), axis=1)
        u = dot_nt(both, lv_nt).reshape(4, cols, levels)
        for s in range(2):
            for h in range(2):
                hs[h, s, k] = u[2 * s : 2 * s + 2, half[h]]

    for c in order:
        for k in range(c * per, (c + 1) * per):
            prepare(k)
        if c == order[0]:
            pl.semaphore_wait(barrier, total)
        first.send_turned(0, c)
        first.send_far(0, c)
        if c != order[0]:
            first.send_near(0, c + 1)
    first.send_near(0, order[-1])
    for c in order:
        first.send_turned(1, c)
    ahead = [(chunks - c) + n_out <= lead for c in range(chunks)]
    for c in order:
        first.send_near(1, c, ahead[c])
    for s in range(2):
        @pl.when(jnp.logical_not(has[s]))
        def _(s=s):
            for ref in (hr, gr, ahalo):
                for h in range(ref.shape[0]):
                    ref[h, s] = jnp.zeros(ref.shape[2:], F32)
            ahalo15[s] = jnp.zeros(ahalo15.shape[1:], F32)
            gr15[s] = jnp.zeros(gr15.shape[1:], F32)

    i = lax.broadcasted_iota(jnp.int32, (size, size), 0)
    j = lax.broadcasted_iota(jnp.int32, (size, size), 1)
    r, r2 = lax.div(i, cols), lax.div(j, cols)
    end = (r == r2) & (((r == 0) & (t == 0)) | ((r == rows - 1) & (t == tiles - 1)))
    row_weight = (band(r - r2) - jnp.where(end, 1.0, 0.0)) * (1.0 / 16.0)
    mm[...] = (row_weight * column_weight(i - r * cols, j - r2 * cols, cols)).astype(BF16)

    stage_refs = ((b0, b01, b02, f0), (b1, b11, b12, f1), (bi, bi1, bi2, fi))
    for ref in (b0, b1, bi):
        ref[...] = jnp.zeros_like(ref)
    copies[3].wait()
    copies[4].wait()

    def lift(b, carry):
        ks = [b * group + g for g in range(group)]
        x = jnp.concatenate([av[k].reshape(size, levels) for k in ks], axis=1)
        hi, lo = split2(dot(mm[...], x))
        bases = []
        for g in range(group):
            part = slice(g * levels, (g + 1) * levels)
            both = jnp.concatenate([hi[:, part], lo[:, part]], axis=1)
            bases.append(dot_nt(both, lv_nt).reshape(rows, cols, levels))
        for v in range(V):
            total = ens[ks[0], v].astype(F32) * bases[0]
            for g in range(1, group):
                total = total + ens[ks[g], v].astype(F32) * bases[g]
            for s in range(2):
                bi[s, v] += total[2 + s * mid : 2 + (s + 1) * mid]
                b0[s, v] += total[edge[s], half[0]]
                b1[s, v] += total[edge[s], half[1]]
        return carry

    lax.fori_loop(0, members // group, lift, 0)

    def to_mate(g):
        part, rec, rec2, full = stage_refs[g]
        return remote(part.at[1 - p], rec, sh_s.at[g, 0], sh_r.at[g, 0], mate, t)

    def to_peer(g, d):
        part, rec, rec2, full = stage_refs[g]
        return remote(part.at[p], rec2.at[d - 1], sh_s.at[g, d], sh_r.at[g, d], lax.rem(m + 2 * d, n), t)

    def back_to_mate(g):
        part, rec, rec2, full = stage_refs[g]
        return remote(full.at[p], full.at[p], sh_s.at[g, n // 2], sh_r.at[g, n // 2], mate, t)

    def back_from_mate(g):
        part, rec, rec2, full = stage_refs[g]
        return remote(full.at[1 - p], full.at[1 - p], sh_s.at[g, n // 2], sh_r.at[g, n // 2], mate, t)

    def reduce_chip(g):
        part, rec, rec2, full = stage_refs[g]
        to_mate(g).wait_recv()
        part[p] += rec[...]
        for d in range(1, n // 2):
            to_peer(g, d).start()

    def reduce_rest(g):
        part, rec, rec2, full = stage_refs[g]
        total = part[p]
        for d in range(1, n // 2):
            to_peer(g, d).wait_recv()
            total = total + rec2[d - 1]
        return total

    def outer_copy(h, s, d):
        here = lax.div(m, 2)
        return remote(stage_refs[h][0].at[p, :, s], iy.at[h, here], ih_s.at[h, d], ih_r.at[h, here],
                      lax.rem(m + 2 * d, n), near[s])

    def outer_send(h):
        for s in range(2):
            @pl.when(has[s] & (p == s))
            def _(s=s):
                for d in range(n // 2):
                    outer_copy(h, s, d).start()

    def outer_recv(h):
        full = stage_refs[h][3]
        for s in range(2):
            @pl.when(has[1 - s] & (p == s))
            def _(s=s):
                total = None
                for d in range(n // 2):
                    remote(iy.at[h, d], iy.at[h, d], ih_s.at[h, 0], ih_r.at[h, d], m, near[1 - s]).wait_recv()
                    total = iy[h, d] if total is None else total + iy[h, d]
                full[s, :, 2] = total

            @pl.when(jnp.logical_not(has[1 - s]) & (p == s))
            def _(s=s):
                full[s, :, 2] = jnp.zeros(full.shape[1:2] + full.shape[3:], F32)

    to_mate(2).start()
    first.forward(0, order[0])
    for k in range(5, 9):
        copies[k].wait()

    place = col[...]
    wide = 2 * cols
    frow = lax.div(place, wide)
    fcol = place - frow * wide
    slot = lax.broadcasted_iota(jnp.int32, (1, slots), 1)
    variable = lax.rem(slot, V)
    early = fcol <= 2 * (ch - 1)
    live = slot < cnt[0]

    def weights(fine, count, shift):
        main = lax.div(fine, 2)
        other = jnp.where(fine - 2 * main == 1, main + 1, main - 1)
        at = lax.broadcasted_iota(jnp.int32, (count, slots), 0) - shift
        return jnp.where(at == main, 0.75, 0.0) + jnp.where(at == other, 0.25, 0.0)

    wr = weights(frow, rows + 2, 1)
    wc = weights(fcol, cols, 0)
    head = w15.shape[0]
    w15[...] = jnp.zeros_like(w15)
    rim = [0, 1, 2, rows - 1, rows, rows + 1]
    lines = rim + list(range(3, rows - 1))
    cut = head + len(rim) * V * ch
    for v in range(V):
        mask = jnp.where(variable == v, 1.0, 0.0)
        for b, a in enumerate(lines):
            start = head + (b * V + v) * ch
            line = wr[a : a + 1, :] * mask
            for h in range(2):
                wt[h, start : start + ch, :] = (wc[half[h]] * line).astype(BF16)
            if b < len(rim):
                w15[b * V + v : b * V + v + 1, :] = wc[ch - 1 : ch] * line
        if v == 0:
            reduce_chip(2)
    wt[1, 0:head, :] = w15[...].astype(BF16)
    for c in order[1:2]:
        first.forward(0, c)
    fi[p] = reduce_rest(2)
    back_to_mate(2).start()

    e15[...] = jnp.zeros_like(e15)
    for s in range(2):
        for w in range(2):
            row = s * (rows - 2) + w
            for v in range(V):
                for k in range(members):
                    e15[s, w, v, k : k + 1, :] = ens[k, v, row, ch - 1 : ch, :].astype(F32)

    def edge_increment(h, c):
        part = stage_refs[h][0]
        sums = [[None] * V for _ in range(2)]
        for k in range(c * per, (c + 1) * per):
            above, below = hr[h, 0, k], hr[h, 1, k]
            fields = (jnp.stack([above[0] + 4.0 * above[1], above[1]]),
                      jnp.stack([below[0], 4.0 * below[0] + below[1]]))
            for s in range(2):
                for v in range(V):
                    term = ens[k, v, edge[s], half[h]].astype(F32) * fields[s]
                    sums[s][v] = term if sums[s][v] is None else sums[s][v] + term
        for s in range(2):
            for v in range(V):
                part[s, v] += sums[s][v]

    hot = lax.broadcasted_iota(jnp.int32, (levels, slots), 0) == lev[...]

    def pick(h, pieces, start):
        flat = jnp.concatenate(pieces, axis=0).reshape(-1, levels)
        both = jnp.concatenate(split2(flat.T), axis=0)
        picked = dot(both, wt[h, start : start + flat.shape[0]])
        return jnp.sum(jnp.where(hot, picked[:levels] + picked[levels:], 0.0), axis=0, keepdims=True)

    def pick_inner(h):
        return pick(h, [fi[s, :, a, half[h]] for s in range(2) for a in range(mid)], cut)

    def pick_rim(h):
        full = stage_refs[h][3]
        return pick(h, [full[1, :, 2], full[0, :, 0], full[0, :, 1], full[1, :, 0], full[1, :, 1], full[0, :, 2]], head)

    def spread(weighted):
        hi, lo = split2(jnp.where(hot, jnp.broadcast_to(weighted, hot.shape), 0.0))
        sent[0:levels, :] = hi
        sent[levels:, :] = lo

    def adjoint(h, start, stop):
        both = dot_nt(wt[h, start:stop, :], sent[...])
        return both[:, :levels] + both[:, levels:]

    def shaped(x):
        return x.reshape(x.shape[0] // (V * ch), V, ch, levels)

    def edge_copy(h, s):
        return remote(adjs.at[h, s], ahalo.at[h, 1 - s], ah_s.at[h], ah_r.at[h, 1 - s], m, near[s])

    def hand_over(h, s):
        return remote(ahalo.at[h, s], ahalo.at[h, s], ah_f.at[h], ah_r.at[h, s], mate, t)

    def single_copy(src, dst, ssem, rsem, s):
        return remote(src.at[s], dst.at[1 - s], ssem.at[s], rsem.at[1 - s], m, near[s])

    def adjoint_edges(h):
        flat = adjoint(h, head * (1 - h), cut)
        thin = flat[:head] if h else None
        rims = shaped(flat[head * h :])
        adjs[h, 0] = rims[0]
        adjs[h, 1] = rims[5]
        if h:
            adjs15[0, 0:V] = thin[0:V]
            adjs15[1, 0:V] = thin[5 * V : 6 * V]
        for s in range(2):
            @pl.when(has[s] & (p == s))
            def _(s=s):
                edge_copy(h, s).start()

            @pl.when(has[s])
            def _(s=s):
                if h:
                    single_copy(adjs15, ahalo15, a15_s, a15_r, s).start()
        for a in range(2):
            adj[:, a, half[h]] = rims[1 + a]
            adj[:, rows - 2 + a, half[h]] = rims[3 + a]
        return thin

    def adjoint_halo(h):
        for s in range(2):
            @pl.when(has[s] & (p == 1 - s))
            def _(s=s):
                hand_over(h, s).wait_recv()
                hand_over(h, s).start()
        for s in range(2):
            @pl.when(has[s] & (p == s))
            def _(s=s):
                hand_over(h, s).wait_recv()
        adj[:, 0, half[h]] += ahalo[h, 0]
        adj[:, rows - 1, half[h]] += ahalo[h, 1]

    def fields(h, outermost):
        where = (0, rows - 1) if outermost else (1, rows - 2)
        weights = [[adj[v, where[s], half[h]] for v in range(V)] for s in range(2)]
        for k in range(members):
            for s in range(2):
                total = ens[k, 0, where[s], half[h]].astype(F32) * weights[s][0]
                for v in range(1, V):
                    total = total + ens[k, v, where[s], half[h]].astype(F32) * weights[s][v]
                gs[2 * h + outermost, s, k] = total

    def chain_open(h):
        first.receive(h)
        for c in order:
            edge_increment(h, c)
        to_mate(h).start()
        reduce_chip(h)
        outer_send(h)

    def chain_close(h, between, after):
        full = stage_refs[h][3]
        full[p, :, 0:2] = reduce_rest(h)
        between()
        outer_recv(h)
        back_to_mate(h).start()
        after()
        back_from_mate(h).wait_recv()

    back_from_mate(2).wait_recv()
    value = pick_inner(0)
    for c in order[2:]:
        first.forward(0, c)
    value = value + pick_inner(1)

    def release(halo, h):
        for c in order:
            halo.send_far(h, c)

    def between_a():
        release(first, 1)
        first.forward(1, order[0])

    chain_open(0)
    for c in order:
        first.send_near(1, c, jnp.logical_not(ahead[c]))
    chain_close(0, between_a, lambda: None)
    for c in order[1:2]:
        first.forward(1, c)
    value = value + pick_rim(0)
    weighted = jnp.where(live & early, wgt[...] * (value - innov[...]), 0.0)
    spread(weighted)
    adjoint_edges(0)
    fields(0, 0)
    for c in order:
        second.send_turned(0, c)
    for c in order:
        second.send_near(0, c, (chunks - c) + n_out <= 4)
    for c in order[2:]:
        first.forward(1, c)

    chain_open(1)
    for c in order:
        second.send_near(0, c, jnp.logical_not((chunks - c) + n_out <= 4))
    adjoint_halo(0)
    fields(0, 1)
    second.send_close(1)
    for c in order[:2]:
        second.forward(0, c)
    chain_close(1, lambda: release(second, 0), lambda: release(second, 1))
    for c in order[2:]:
        second.forward(0, c)
    value = value + pick_rim(1)
    spread(jnp.where(live, wgt[...] * (value - innov[...]), 0.0))
    thin = adjoint_edges(1)
    fields(1, 0)
    second.send_close(2)
    for c in order:
        second.forward(1, c)
    for h in range(2):
        inner = shaped(adjoint(h, cut, wt.shape[1]))
        for a in range(rows - 4):
            adj[:, 2 + a, half[h]] = inner[a]
    adjoint_halo(1)
    for s in range(2):
        @pl.when(has[s])
        def _(s=s):
            remote(ahalo15.at[s], ahalo15.at[s], a15_s.at[s], a15_r.at[s], m, near[s]).wait_recv()
    for s in range(2):
        for w in range(2):
            a = 1 + 2 * s + w
            line = thin[a * V : (a + 1) * V]
            if w == s:
                line = line + ahalo15[s, 0:V]
            total = e15[s, w, 0] * line[0:1]
            for v in range(1, V):
                total = total + e15[s, w, v] * line[v : v + 1]
            gs15[s, w] = total
            for v in range(V):
                adj[v, s * (rows - 2) + w, ch - 1 : ch, :] = line[v : v + 1]
    for s in range(2):
        @pl.when(has[s])
        def _(s=s):
            single_copy(gs15, gr15, g15_s, g15_r, s).start()
    fields(1, 1)
    for c in order:
        second.send_far(2, c)
    second.send_close(3)
    for c in order:
        second.send_far(3, c)

    pair = group

    def inside(b, carry):
        ks = [b * pair + g for g in range(pair)]
        parts = []
        for k in ks:
            total = ens[k, 0].astype(F32) * adj[0]
            for v in range(1, V):
                total = total + ens[k, v].astype(F32) * adj[v]
            parts.append(total.reshape(size, levels))
        hi, lo = split2(jnp.concatenate(parts, axis=1))
        hi, lo = split2(dot(mm[...], hi) + dot(mm[...], lo))
        for g, k in enumerate(ks):
            part = slice(g * levels, (g + 1) * levels)
            both = jnp.concatenate([hi[:, part], lo[:, part]], axis=1)
            out[k] = av[k].astype(F32) + dot(both, lv_nn).reshape(rows, cols, levels)
        return carry

    steps = members // pair
    stops = [0, steps // 5, 2 * steps // 5, steps]
    lax.fori_loop(stops[0], stops[1], inside, 0)
    for c in order[:2]:
        second.forward(2, c)
    lax.fori_loop(stops[1], stops[2], inside, 0)
    for c in order[2:]:
        second.forward(2, c)
    lax.fori_loop(stops[2], stops[3], inside, 0)

    def outer_early(b, carry):
        ks = [b * pair + g for g in range(pair)]
        parts = []
        for k in ks:
            sides = []
            for s in range(2):
                for o in ((0, 1) if s == 0 else (1, 0)):
                    at = lax.broadcasted_iota(jnp.int32, (ch, levels), 0)
                    sides.append(jnp.where(at == ch - 1, 0.0, gr[o, s, k]))
                    sides.append(gr[2, s, k] if o == 0 else jnp.zeros((ch, levels), F32))
            parts.append(jnp.concatenate(sides, axis=0))
        back = dot(em[...], jnp.concatenate(split2(jnp.concatenate(parts, axis=1)), axis=0))
        hi, lo = split2(back)
        for g, k in enumerate(ks):
            part = slice(g * levels, (g + 1) * levels)
            both = jnp.concatenate([hi[:, part], lo[:, part]], axis=1)
            add = dot(both, lv_nn).reshape(4, cols, levels)
            out[k, 0:2] += add[0:2]
            out[k, rows - 2 : rows] += add[2:4]
        return carry

    for c in order[:1]:
        second.forward(3, c)
    second.receive(0)
    third = steps // 3
    lax.fori_loop(0, third, outer_early, 0)
    for c in order[1:2]:
        second.forward(3, c)
    lax.fori_loop(third, 2 * third, outer_early, 0)
    for c in order[2:]:
        second.forward(3, c)
    lax.fori_loop(2 * third, steps, outer_early, 0)

    i = lax.broadcasted_iota(jnp.int32, (4 * cols, 2 * ch + 16), 0)
    j = lax.broadcasted_iota(jnp.int32, (4 * cols, 2 * ch + 16), 1)
    q = lax.div(i, cols)
    r = jnp.where(q < 2, q, q + rows - 4)
    spot = j - 2 * ch
    r2 = jnp.where(spot < 0, jnp.where(j < ch, -1, rows), jnp.where(spot < 2, spot - 2, spot - 2 + rows))
    c2 = jnp.where(spot < 0, jnp.where(j < ch, j, j - ch) + ch, ch - 1)
    last = band(r - r2) * (1.0 / 16.0) * column_weight(i - q * cols, c2, cols)
    last = jnp.where(spot < 4, last, 0.0).astype(BF16)
    last = jnp.concatenate([last, last], axis=1)

    for s in range(2):
        @pl.when(has[s])
        def _(s=s):
            remote(gr15.at[s], gr15.at[s], g15_s.at[s], g15_r.at[s], m, near[s]).wait_recv()
    blank = jnp.zeros((12, levels), F32)

    def outer_late(c):
        ks = list(range(c * per, (c + 1) * per))
        rowsets = []
        for k in ks:
            rowsets += [gr[3, 0, k], gr[3, 1, k]] + [gr15[s, w, k : k + 1] for s in range(2) for w in range(2)] + [blank]
        both = jnp.concatenate(split2(jnp.concatenate(rowsets, axis=0)), axis=1)
        hi, lo = split2(dot(both, lv_nn))
        span = 2 * ch + 16
        stack = jnp.concatenate(
            [jnp.concatenate([x[g * span : (g + 1) * span] for g in range(len(ks))], axis=1) for x in (hi, lo)], axis=0)
        add = dot(last, stack)
        for g, k in enumerate(ks):
            piece = add[:, g * levels : (g + 1) * levels].reshape(4, cols, levels)
            out[k, 0:2] += piece[0:2]
            out[k, rows - 2 : rows] += piece[2:4]

    for c in order:
        second.receive_chunk(3, c)
        outer_late(c)

    first.drain()
    second.drain()
    for g in range(3):
        to_mate(g).wait_send()
        for d in range(1, n // 2):
            to_peer(g, d).wait_send()
        back_to_mate(g).wait_send()
    for h in range(2):
        for s in range(2):
            @pl.when(has[s] & (p == s))
            def _(h=h, s=s):
                for d in range(n // 2):
                    outer_copy(h, s, d).wait_send()

            @pl.when(has[s] & (p == s))
            def _(h=h, s=s):
                edge_copy(h, s).wait_send()

            @pl.when(has[s] & (p == 1 - s))
            def _(h=h, s=s):
                hand_over(h, s).wait_send()
    for s in range(2):
        @pl.when(has[s])
        def _(s=s):
            single_copy(adjs15, ahalo15, a15_s, a15_r, s).wait_send()
            single_copy(gs15, gr15, g15_s, g15_r, s).wait_send()


def solution(mesh):
    n = mesh.shape["mem"]
    tiles = mesh.shape["tile"]

    def on_device(alpha, ensemble, loc_vert, obs_col, obs_lev, obs_count, innovation, obs_weight):
        members, rows, cols, levels = alpha.shape
        slots = obs_col.shape[1]
        chunks = 4 if members % 4 == 0 else 1
        ch = cols // 2
        mid = (rows - 4) // 2
        vmem = pl.BlockSpec(memory_space=pltpu.VMEM)
        hbm = pl.BlockSpec(memory_space=pltpu.HBM)
        turned = pltpu.VMEM((2, 2, members, 2, ch, levels), F32)
        passing = pltpu.VMEM((2, members, 2, ch, levels), F32)
        line2 = pltpu.VMEM((4, 2, members, ch, levels), F32)
        passing2 = pltpu.VMEM((4, members, ch, levels), F32)
        dma = pltpu.SemaphoreType.DMA
        line = pltpu.VMEM((1, slots), F32)
        mark = pltpu.VMEM((1, slots), jnp.int32)
        padded = -(-members // 8) * 8
        thin = -(-6 * V // 16) * 16

        def sums(piece, result):
            return [pltpu.VMEM((2,) + piece, F32), pltpu.VMEM(piece, F32),
                    pltpu.VMEM((max(n // 2 - 1, 1),) + piece, F32), pltpu.VMEM((2,) + result, F32)]

        borders = pltpu.VMEM((2, 2, V, ch, levels), F32)
        small = pltpu.VMEM((2, 8, levels), F32)
        slim = pltpu.VMEM((2, 2, padded, levels), F32)
        return pl.pallas_call(
            functools.partial(kernel, n, tiles, chunks),
            out_shape=jax.ShapeDtypeStruct(alpha.shape, F32),
            in_specs=[hbm, hbm, hbm, hbm, hbm, pl.BlockSpec(memory_space=pltpu.SMEM), hbm, hbm],
            out_specs=vmem,
            scratch_shapes=[
                pltpu.VMEM(alpha.shape, BF16), pltpu.VMEM(ensemble.shape, BF16),
                pltpu.VMEM(loc_vert.shape, BF16), mark, mark, line, line,
                turned, turned, passing, line2, line2, passing2,
                pltpu.VMEM((rows * cols, rows * cols), BF16),
                pltpu.VMEM((4 * cols, 4 * cols), BF16),
                pltpu.VMEM((4 * cols, 8 * cols), BF16),
                pltpu.VMEM((2, thin + V * (rows + 2) * ch, slots), BF16),
                pltpu.VMEM((thin, slots), F32),
                pltpu.VMEM((2 * levels, slots), BF16),
                pltpu.VMEM((2, 2, V, padded, levels), F32),
                *sums((V, mid, cols, levels), (V, mid, cols, levels)),
                *sums((V, 2, ch, levels), (V, 3, ch, levels)), *sums((V, 2, ch, levels), (V, 3, ch, levels)),
                pltpu.VMEM((2, n // 2, V, ch, levels), F32), pltpu.VMEM((V, rows, cols, levels), F32), borders, borders,
                small, small, slim, slim,
                dma((9,)),
                dma((2,)), dma((2, 2)), dma((1,)), dma((2, chunks)),
                dma((2,)), dma((1, 2)), dma((2, chunks)), dma((1,)), dma((4, chunks)),
                dma((3, n // 2 + 1)), dma((3, n // 2 + 1)),
                dma((2, n // 2)), dma((2, n // 2)), dma((2,)), dma((2, 2)), dma((2,)),
                dma((2,)), dma((2,)), dma((2,)), dma((2,)),
            ],
            compiler_params=pltpu.CompilerParams(
                collective_id=0, has_side_effects=True, vmem_limit_bytes=48 << 20),
        )(*[pltpu.with_memory_space_constraint(x, pltpu.HBM) for x in (alpha, ensemble, loc_vert, obs_col, obs_lev)],
          obs_count, *[pltpu.with_memory_space_constraint(x, pltpu.HBM) for x in (innovation, obs_weight)])

    in_specs = (
        P("mem", "tile", None, None),
        P("mem", None, "tile", None, None),
        P(),
        P("tile", None),
        P("tile", None),
        P("tile"),
        P("tile", None),
        P("tile", None),
    )
    out_specs = P("mem", "tile", None, None)
    return jax.shard_map(
        on_device, mesh=mesh, in_specs=in_specs, out_specs=out_specs, check_vma=False
    )
```

```python
import functools

import jax
import jax.numpy as jnp
from jax import lax
from jax.experimental import pallas as pl
from jax.experimental.pallas import tpu as pltpu
from jax.sharding import PartitionSpec as P

V = 3
F32 = jnp.float32
BF16 = jnp.bfloat16
MESH = pl.DeviceIdType.MESH


def split2(x):
    hi = x.astype(BF16)
    lo = (x - hi.astype(F32)).astype(BF16)
    return hi, lo


def dot(a, b):
    return jnp.dot(a, b, preferred_element_type=F32)


def dot_nt(a, b):
    return lax.dot_general(a, b, (((1,), (1,)), ((), ())), preferred_element_type=F32)


def band(distance):
    d = jnp.abs(distance)
    return jnp.where(d == 0, 6.0, jnp.where(d == 1, 4.0, jnp.where(d == 2, 1.0, 0.0)))


def column_weight(c, c2, cols):
    end = (c == c2) & ((c == 0) | (c == cols - 1))
    return (band(c - c2) - jnp.where(end, 1.0, 0.0)) * (1.0 / 16.0)


def kernel(n, tiles, chunks, alpha_h, ens_h, loc_h, col_h, lev_h, cnt, innov_h, wgt_h, out,
           av, ens, loc, col, lev, innov, wgt,
           hs, hr, hl, gs, gr, gl, mm, sc, em, el, wt, w15, sent, e15,
           bi, bi1, bi2, fi, b0, b01, b02, f0, b1, b11, b12, f1,
           iy, adj, adjs, ahalo, adjs15, ahalo15, gs15, gr15,
           in_sem, hs_s, hs_r, hl_s, hl_r, gs_s, gs_r, ge_r, gl_s, gl_r,
           sh_s, sh_r, ih_s, ih_r, ah_s, ah_r, ah_f, a15_s, a15_r, g15_s, g15_r):
    members, rows, cols, levels = out.shape
    size = rows * cols
    ch = cols // 2
    mid = (rows - 4) // 2
    per = members // chunks
    group = 4 if members % 4 == 0 else 1
    slots = col.shape[1]
    m = lax.axis_index("mem")
    t = lax.axis_index("tile")
    p = lax.rem(m, 2)
    mate = m + 1 - 2 * p
    has = (t > 0, t < tiles - 1)
    near = (t - 1, t + 1)
    edge = (slice(0, 2), slice(rows - 2, rows))
    half = (slice(0, ch), slice(ch, cols))

    def loads():
        pairs = (
            (alpha_h.at[:, 0:2], av.at[:, 0:2]),
            (alpha_h.at[:, rows - 2 : rows], av.at[:, rows - 2 : rows]),
            (loc_h, loc),
            (alpha_h.at[:, 2 : rows - 2], av.at[:, 2 : rows - 2]),
            (ens_h, ens),
            (col_h, col), (lev_h, lev), (innov_h, innov), (wgt_h, wgt))
        return [pltpu.make_async_copy(a, b, in_sem.at[i]) for i, (a, b) in enumerate(pairs)]

    copies = loads()
    for copy in copies:
        copy.start()

    relays = tiles % 2 == 0 and tiles >= 4
    lead = chunks // 2
    odd = lax.rem(t, 2)
    turn = tiles // 2
    share_out = lax.div(chunks * lax.div(t + odd, 2), max(turn, 1))
    n_out = odd * (chunks - share_out) + (1 - odd) * share_out
    share_in = lax.div(chunks * lax.div(t + 2 - 3 * odd, 2), max(turn, 1))
    n_in = (1 - odd) * (chunks - share_in) + odd * share_in
    far = (t >= 2, t <= tiles - 3)
    passes = jnp.where(odd == 1, t - 2, tiles - 3 - t) >= 0

    barrier = pltpu.get_barrier_semaphore()

    def greet(who, where):
        pl.semaphore_signal(barrier, inc=1, device_id={"mem": who, "tile": where}, device_id_type=MESH)

    for d in range(1, n):
        greet(lax.rem(m + d, n), t)
    total = jnp.int32(n - 1)
    for s in range(2):
        @pl.when(has[s])
        def _(s=s):
            for d in range(n // 2):
                greet(lax.rem(m + 2 * d, n), near[s])
        total = total + (n // 2) * has[s].astype(jnp.int32)
        if relays:
            @pl.when(far[s])
            def _(s=s):
                greet(m, t - 2 + 4 * s)
            total = total + far[s].astype(jnp.int32)

    def remote(src, dst, ssem, rsem, who, where):
        return pltpu.make_async_remote_copy(
            src_ref=src, dst_ref=dst, send_sem=ssem, recv_sem=rsem,
            device_id={"mem": who, "tile": where}, device_id_type=MESH)

    class Halo:
        def __init__(self, src, dst, via, ss, sr, vs, vr, groups, fine=None):
            self.src, self.dst, self.via = src, dst, via
            self.ss, self.sr, self.vs, self.vr = ss, sr, vs, vr
            self.groups, self.fine = groups, fine

        def group(self, h):
            return [b for b, span in enumerate(self.groups) if span[0] <= h < span[1]][0]

        def landed(self, h, s, c):
            if self.fine is not None and h == self.src.shape[0] - 1:
                return self.fine.at[s, c]
            return self.sr.at[self.group(h), s]

        def direct(self, h, s, c):
            part = pl.ds(c * per, per)
            return remote(self.src.at[h, s, part], self.dst.at[h, 1 - s, part],
                          self.ss.at[s], self.landed(h, 1 - s, c), m, near[s])

        def receive_chunk(self, h, c):
            for s in range(2):
                @pl.when(has[s])
                def _(s=s):
                    part = self.dst.at[h, s, pl.ds(c * per, per)]
                    remote(part, part, self.ss.at[s], self.landed(h, s, c), m, near[s]).wait_recv()

        def detour(self, h, s, c):
            part = pl.ds(c * per, per)
            return remote(self.src.at[h, s, part], self.via.at[h, part],
                          self.ss.at[s], self.vr.at[h, c], m, t + 1 - 2 * odd)

        def onward(self, h, c):
            part = pl.ds(c * per, per)
            return remote(self.via.at[h, part], self.dst.at[h, odd, part],
                          self.vs.at[0], self.landed(h, odd, c), m, t + 2 - 4 * odd)

        def send_turned(self, h, c):
            for s in range(2):
                if relays:
                    @pl.when(has[s] & (odd == s) & (c >= chunks - n_out))
                    def _(s=s):
                        self.detour(h, s, c).start()

        def send_far(self, h, c):
            for s in range(2):
                straight = c < chunks - n_out if relays else True

                @pl.when(has[s] & (odd == s) & straight)
                def _(s=s):
                    self.direct(h, s, c).start()

        def send_near(self, h, c, when=True):
            for s in range(2):
                @pl.when(has[s] & (odd != s) & when)
                def _(s=s):
                    self.direct(h, s, c).start()

        def send_close(self, h):
            for c in order:
                self.send_turned(h, c)
            for c in order:
                self.send_near(h, c)

        def forward(self, h, c):
            if relays:
                @pl.when(passes & (c >= chunks - n_in))
                def _():
                    self.onward_recv(h, c).wait_recv()
                    self.onward(h, c).start()

        def onward_recv(self, h, c):
            part = pl.ds(c * per, per)
            return remote(self.via.at[h, part], self.via.at[h, part],
                          self.vs.at[0], self.vr.at[h, c], m, t + 1 - 2 * odd)

        def receive(self, b):
            span = self.groups[b]
            for s in range(2):
                @pl.when(has[s])
                def _(s=s):
                    every = self.dst.at[span[0] : span[1], s]
                    remote(every, every, self.ss.at[s], self.sr.at[b, s], m, near[s]).wait_recv()

        def drain(self):
            for s in range(2):
                @pl.when(has[s])
                def _(s=s):
                    remote(self.src.at[:, s], self.dst.at[:, s], self.ss.at[s], self.sr.at[0, s], m, near[s]).wait_send()
            if relays:
                for count in range(1, chunks + 1):
                    @pl.when(passes & (n_in == count))
                    def _(count=count):
                        every = self.via.at[:, members - count * per : members]
                        remote(every, every, self.vs.at[0], self.sr.at[0, 0], m, t + 2 - 4 * odd).wait_send()

    first = Halo(hs, hr, hl, hs_s, hs_r, hl_s, hl_r, ((0, 1), (1, 2)))
    second = Halo(gs, gr, gl, gs_s, gs_r, gl_s, gl_r, ((0, 3),), ge_r)
    order = list(range(chunks - 1, -1, -1))

    i = lax.broadcasted_iota(jnp.int32, (4 * cols, 4 * cols), 0)
    j = lax.broadcasted_iota(jnp.int32, (4 * cols, 4 * cols), 1)
    q, q2 = lax.div(i, cols), lax.div(j, cols)
    across = column_weight(i - q * cols, j - q2 * cols, cols)
    sc[...] = (jnp.where(q == q2, 1.0 / 16.0, 0.0) * across).astype(BF16)
    r = jnp.where(q < 2, q, q + rows - 4)
    r2 = jnp.where(q2 < 2, q2 - 2, q2 - 2 + rows)
    corner = (band(r - r2) * (1.0 / 16.0) * across).astype(BF16)
    em[:, 0 : 4 * cols] = corner
    em[:, 4 * cols :] = corner

    for k in range(3):
        copies[k].wait()
    lv = loc[...]
    lv_nt = jnp.concatenate([lv, lv], axis=1)
    lv_nn = jnp.concatenate([lv, lv], axis=0)

    def prepare(k):
        x = jnp.concatenate([av[k, 0:2], av[k, rows - 2 : rows]], axis=0).reshape(4 * cols, levels)
        both = jnp.concatenate(split2(dot(sc[...], x)), axis=1)
        u = dot_nt(both, lv_nt).reshape(4, cols, levels)
        for s in range(2):
            for h in range(2):
                hs[h, s, k] = u[2 * s : 2 * s + 2, half[h]]

    for c in order:
        for k in range(c * per, (c + 1) * per):
            prepare(k)
        if c == order[0]:
            pl.semaphore_wait(barrier, total)
        first.send_turned(0, c)
        first.send_far(0, c)
        if c != order[0]:
            first.send_near(0, c + 1)
    first.send_near(0, order[-1])
    for c in order:
        first.send_turned(1, c)
    ahead = [(chunks - c) + n_out <= lead for c in range(chunks)]
    for c in order:
        first.send_near(1, c, ahead[c])
    for s in range(2):
        @pl.when(jnp.logical_not(has[s]))
        def _(s=s):
            for ref in (hr, gr, ahalo):
                for h in range(ref.shape[0]):
                    ref[h, s] = jnp.zeros(ref.shape[2:], F32)
            ahalo15[s] = jnp.zeros(ahalo15.shape[1:], F32)
            gr15[s] = jnp.zeros(gr15.shape[1:], F32)

    i = lax.broadcasted_iota(jnp.int32, (size, size), 0)
    j = lax.broadcasted_iota(jnp.int32, (size, size), 1)
    r, r2 = lax.div(i, cols), lax.div(j, cols)
    end = (r == r2) & (((r == 0) & (t == 0)) | ((r == rows - 1) & (t == tiles - 1)))
    row_weight = (band(r - r2) - jnp.where(end, 1.0, 0.0)) * (1.0 / 16.0)
    mm[...] = (row_weight * column_weight(i - r * cols, j - r2 * cols, cols)).astype(BF16)

    stage_refs = ((b0, b01, b02, f0), (b1, b11, b12, f1), (bi, bi1, bi2, fi))
    for ref in (b0, b1, bi):
        ref[...] = jnp.zeros_like(ref)
    copies[3].wait()
    copies[4].wait()

    def lift(b, carry):
        ks = [b * group + g for g in range(group)]
        x = jnp.concatenate([av[k].reshape(size, levels) for k in ks], axis=1)
        hi, lo = split2(dot(mm[...], x))
        bases = []
        for g in range(group):
            part = slice(g * levels, (g + 1) * levels)
            both = jnp.concatenate([hi[:, part], lo[:, part]], axis=1)
            bases.append(dot_nt(both, lv_nt).reshape(rows, cols, levels))
        for v in range(V):
            total = ens[ks[0], v].astype(F32) * bases[0]
            for g in range(1, group):
                total = total + ens[ks[g], v].astype(F32) * bases[g]
            for s in range(2):
                bi[s, v] += total[2 + s * mid : 2 + (s + 1) * mid]
                b0[s, v] += total[edge[s], half[0]]
                b1[s, v] += total[edge[s], half[1]]
        return carry

    lax.fori_loop(0, members // group, lift, 0)

    def to_mate(g):
        part, rec, rec2, full = stage_refs[g]
        return remote(part.at[1 - p], rec, sh_s.at[g, 0], sh_r.at[g, 0], mate, t)

    def to_peer(g, d):
        part, rec, rec2, full = stage_refs[g]
        return remote(part.at[p], rec2.at[d - 1], sh_s.at[g, d], sh_r.at[g, d], lax.rem(m + 2 * d, n), t)

    def back_to_mate(g):
        part, rec, rec2, full = stage_refs[g]
        return remote(full.at[p], full.at[p], sh_s.at[g, n // 2], sh_r.at[g, n // 2], mate, t)

    def back_from_mate(g):
        part, rec, rec2, full = stage_refs[g]
        return remote(full.at[1 - p], full.at[1 - p], sh_s.at[g, n // 2], sh_r.at[g, n // 2], mate, t)

    def reduce_chip(g):
        part, rec, rec2, full = stage_refs[g]
        to_mate(g).wait_recv()
        part[p] += rec[...]
        for d in range(1, n // 2):
            to_peer(g, d).start()

    def reduce_rest(g):
        part, rec, rec2, full = stage_refs[g]
        total = part[p]
        for d in range(1, n // 2):
            to_peer(g, d).wait_recv()
            total = total + rec2[d - 1]
        return total

    def outer_copy(h, s, d):
        here = lax.div(m, 2)
        return remote(stage_refs[h][0].at[p, :, s], iy.at[h, here], ih_s.at[h, d], ih_r.at[h, here],
                      lax.rem(m + 2 * d, n), near[s])

    def outer_send(h):
        for s in range(2):
            @pl.when(has[s] & (p == s))
            def _(s=s):
                for d in range(n // 2):
                    outer_copy(h, s, d).start()

    def outer_recv(h):
        full = stage_refs[h][3]
        for s in range(2):
            @pl.when(has[1 - s] & (p == s))
            def _(s=s):
                total = None
                for d in range(n // 2):
                    remote(iy.at[h, d], iy.at[h, d], ih_s.at[h, 0], ih_r.at[h, d], m, near[1 - s]).wait_recv()
                    total = iy[h, d] if total is None else total + iy[h, d]
                full[s, :, 2] = total

            @pl.when(jnp.logical_not(has[1 - s]) & (p == s))
            def _(s=s):
                full[s, :, 2] = jnp.zeros(full.shape[1:2] + full.shape[3:], F32)

    to_mate(2).start()
    first.forward(0, order[0])
    for k in range(5, 9):
        copies[k].wait()

    place = col[...]
    wide = 2 * cols
    frow = lax.div(place, wide)
    fcol = place - frow * wide
    slot = lax.broadcasted_iota(jnp.int32, (1, slots), 1)
    variable = lax.rem(slot, V)
    early = fcol <= 2 * (ch - 1)
    live = slot < cnt[0]

    def weights(fine, count, shift):
        main = lax.div(fine, 2)
        other = jnp.where(fine - 2 * main == 1, main + 1, main - 1)
        at = lax.broadcasted_iota(jnp.int32, (count, slots), 0) - shift
        return jnp.where(at == main, 0.75, 0.0) + jnp.where(at == other, 0.25, 0.0)

    wr = weights(frow, rows + 2, 1)
    wc = weights(fcol, cols, 0)
    head = w15.shape[0]
    w15[...] = jnp.zeros_like(w15)
    rim = [0, 1, 2, rows - 1, rows, rows + 1]
    lines = rim + list(range(3, rows - 1))
    cut = head + len(rim) * V * ch
    for v in range(V):
        mask = jnp.where(variable == v, 1.0, 0.0)
        for b, a in enumerate(lines):
            start = head + (b * V + v) * ch
            line = wr[a : a + 1, :] * mask
            for h in range(2):
                wt[h, start : start + ch, :] = (wc[half[h]] * line).astype(BF16)
            if b < len(rim):
                w15[b * V + v : b * V + v + 1, :] = wc[ch - 1 : ch] * line
        if v == 0:
            reduce_chip(2)
    wt[1, 0:head, :] = w15[...].astype(BF16)
    for c in order[1:2]:
        first.forward(0, c)
    fi[p] = reduce_rest(2)
    back_to_mate(2).start()

    i = lax.broadcasted_iota(jnp.int32, (4 * cols, 2 * ch + 16), 0)
    j = lax.broadcasted_iota(jnp.int32, (4 * cols, 2 * ch + 16), 1)
    q = lax.div(i, cols)
    r = jnp.where(q < 2, q, q + rows - 4)
    spot = j - 2 * ch
    r2 = jnp.where(spot < 0, jnp.where(j < ch, -1, rows), jnp.where(spot < 2, spot - 2, spot - 2 + rows))
    c2 = jnp.where(spot < 0, jnp.where(j < ch, j, j - ch) + ch, ch - 1)
    last = band(r - r2) * (1.0 / 16.0) * column_weight(i - q * cols, c2, cols)
    last = jnp.where(spot < 4, last, 0.0).astype(BF16)
    el[:, 0 : 2 * ch + 16] = last
    el[:, 2 * ch + 16 :] = last

    e15[...] = jnp.zeros_like(e15)
    for s in range(2):
        for w in range(2):
            row = s * (rows - 2) + w
            for v in range(V):
                for k in range(members):
                    e15[s, w, v, k : k + 1, :] = ens[k, v, row, ch - 1 : ch, :].astype(F32)

    def edge_increment(h, c):
        part = stage_refs[h][0]
        sums = [[None] * V for _ in range(2)]
        for k in range(c * per, (c + 1) * per):
            above, below = hr[h, 0, k], hr[h, 1, k]
            fields = (jnp.stack([above[0] + 4.0 * above[1], above[1]]),
                      jnp.stack([below[0], 4.0 * below[0] + below[1]]))
            for s in range(2):
                for v in range(V):
                    term = ens[k, v, edge[s], half[h]].astype(F32) * fields[s]
                    sums[s][v] = term if sums[s][v] is None else sums[s][v] + term
        for s in range(2):
            for v in range(V):
                part[s, v] += sums[s][v]

    hot = lax.broadcasted_iota(jnp.int32, (levels, slots), 0) == lev[...]

    def pick(h, pieces, start):
        flat = jnp.concatenate(pieces, axis=0).reshape(-1, levels)
        both = jnp.concatenate(split2(flat.T), axis=0)
        picked = dot(both, wt[h, start : start + flat.shape[0]])
        return jnp.sum(jnp.where(hot, picked[:levels] + picked[levels:], 0.0), axis=0, keepdims=True)

    def pick_inner(h):
        return pick(h, [fi[s, :, a, half[h]] for s in range(2) for a in range(mid)], cut)

    def pick_rim(h):
        full = stage_refs[h][3]
        return pick(h, [full[1, :, 2], full[0, :, 0], full[0, :, 1], full[1, :, 0], full[1, :, 1], full[0, :, 2]], head)

    def spread(weighted):
        hi, lo = split2(jnp.where(hot, jnp.broadcast_to(weighted, hot.shape), 0.0))
        sent[0:levels, :] = hi
        sent[levels:, :] = lo

    def adjoint(h, start, stop):
        both = dot_nt(wt[h, start:stop, :], sent[...])
        return both[:, :levels] + both[:, levels:]

    def shaped(x):
        return x.reshape(x.shape[0] // (V * ch), V, ch, levels)

    def edge_copy(h, s):
        return remote(adjs.at[h, s], ahalo.at[h, 1 - s], ah_s.at[h], ah_r.at[h, 1 - s], m, near[s])

    def hand_over(h, s):
        return remote(ahalo.at[h, s], ahalo.at[h, s], ah_f.at[h], ah_r.at[h, s], mate, t)

    def single_copy(src, dst, ssem, rsem, s):
        return remote(src.at[s], dst.at[1 - s], ssem.at[s], rsem.at[1 - s], m, near[s])

    def adjoint_edges(h):
        flat = adjoint(h, head * (1 - h), cut)
        thin = flat[:head] if h else None
        rims = shaped(flat[head * h :])
        adjs[h, 0] = rims[0]
        adjs[h, 1] = rims[5]
        if h:
            adjs15[0, 0:V] = thin[0:V]
            adjs15[1, 0:V] = thin[5 * V : 6 * V]
        for s in range(2):
            @pl.when(has[s] & (p == s))
            def _(s=s):
                edge_copy(h, s).start()

            @pl.when(has[s])
            def _(s=s):
                if h:
                    single_copy(adjs15, ahalo15, a15_s, a15_r, s).start()
        for a in range(2):
            adj[:, a, half[h]] = rims[1 + a]
            adj[:, rows - 2 + a, half[h]] = rims[3 + a]
        return thin

    def adjoint_halo(h):
        for s in range(2):
            @pl.when(has[s] & (p == 1 - s))
            def _(s=s):
                hand_over(h, s).wait_recv()
                hand_over(h, s).start()
        for s in range(2):
            @pl.when(has[s] & (p == s))
            def _(s=s):
                hand_over(h, s).wait_recv()
        adj[:, 0, half[h]] += ahalo[h, 0]
        adj[:, rows - 1, half[h]] += ahalo[h, 1]

    def fields(h, outermost):
        where = (0, rows - 1) if outermost else (1, rows - 2)
        weights = [[adj[v, where[s], half[h]] for v in range(V)] for s in range(2)]
        for k in range(members):
            for s in range(2):
                total = ens[k, 0, where[s], half[h]].astype(F32) * weights[s][0]
                for v in range(1, V):
                    total = total + ens[k, v, where[s], half[h]].astype(F32) * weights[s][v]
                gs[2 * h + outermost, s, k] = total

    def chain_open(h):
        first.receive(h)
        for c in order:
            edge_increment(h, c)
        to_mate(h).start()
        reduce_chip(h)
        outer_send(h)

    def chain_close(h, between, after):
        full = stage_refs[h][3]
        full[p, :, 0:2] = reduce_rest(h)
        between()
        outer_recv(h)
        back_to_mate(h).start()
        after()
        back_from_mate(h).wait_recv()

    back_from_mate(2).wait_recv()
    value = pick_inner(0)
    for c in order[2:]:
        first.forward(0, c)
    value = value + pick_inner(1)

    def release(halo, h):
        for c in order:
            halo.send_far(h, c)

    def between_a():
        release(first, 1)
        first.forward(1, order[0])

    chain_open(0)
    for c in order:
        first.send_near(1, c, jnp.logical_not(ahead[c]))
    chain_close(0, between_a, lambda: None)
    for c in order[1:2]:
        first.forward(1, c)
    value = value + pick_rim(0)
    weighted = jnp.where(live & early, wgt[...] * (value - innov[...]), 0.0)
    spread(weighted)
    adjoint_edges(0)
    fields(0, 0)
    early_near = [(chunks - c) + n_out <= chunks for c in range(chunks)]
    for c in order:
        second.send_turned(0, c)
    for c in order:
        second.send_near(0, c, early_near[c])
    for c in order[2:]:
        first.forward(1, c)

    chain_open(1)
    for c in order:
        second.send_near(0, c, jnp.logical_not(early_near[c]))
    adjoint_halo(0)
    fields(0, 1)
    second.send_close(1)
    for c in order[:2]:
        second.forward(0, c)
    chain_close(1, lambda: release(second, 0), lambda: release(second, 1))
    for c in order[2:]:
        second.forward(0, c)
    value = value + pick_rim(1)
    spread(jnp.where(live, wgt[...] * (value - innov[...]), 0.0))
    thin = adjoint_edges(1)
    fields(1, 0)
    second.send_close(2)
    for c in order:
        second.forward(1, c)
    for h in range(2):
        inner = shaped(adjoint(h, cut, wt.shape[1]))
        for a in range(rows - 4):
            adj[:, 2 + a, half[h]] = inner[a]
    adjoint_halo(1)
    for s in range(2):
        @pl.when(has[s])
        def _(s=s):
            remote(ahalo15.at[s], ahalo15.at[s], a15_s.at[s], a15_r.at[s], m, near[s]).wait_recv()
    for s in range(2):
        for w in range(2):
            a = 1 + 2 * s + w
            line = thin[a * V : (a + 1) * V]
            if w == s:
                line = line + ahalo15[s, 0:V]
            total = e15[s, w, 0] * line[0:1]
            for v in range(1, V):
                total = total + e15[s, w, v] * line[v : v + 1]
            gs15[s, w] = total
            for v in range(V):
                adj[v, s * (rows - 2) + w, ch - 1 : ch, :] = line[v : v + 1]
    for s in range(2):
        @pl.when(has[s])
        def _(s=s):
            single_copy(gs15, gr15, g15_s, g15_r, s).start()
    fields(1, 1)
    for c in order:
        second.send_far(2, c)
    second.send_close(3)
    for c in order:
        second.send_far(3, c)

    pair = group

    def inside(b, carry):
        ks = [b * pair + g for g in range(pair)]
        parts = []
        for k in ks:
            total = ens[k, 0].astype(F32) * adj[0]
            for v in range(1, V):
                total = total + ens[k, v].astype(F32) * adj[v]
            parts.append(total.reshape(size, levels))
        hi, lo = split2(jnp.concatenate(parts, axis=1))
        hi, lo = split2(dot(mm[...], hi) + dot(mm[...], lo))
        for g, k in enumerate(ks):
            part = slice(g * levels, (g + 1) * levels)
            both = jnp.concatenate([hi[:, part], lo[:, part]], axis=1)
            out[k] = av[k].astype(F32) + dot(both, lv_nn).reshape(rows, cols, levels)
        return carry

    steps = members // pair
    stops = [0, steps // 5, 2 * steps // 5, steps]
    lax.fori_loop(stops[0], stops[1], inside, 0)
    for c in order[:2]:
        second.forward(2, c)
    lax.fori_loop(stops[1], stops[2], inside, 0)
    for c in order[2:]:
        second.forward(2, c)
    lax.fori_loop(stops[2], stops[3], inside, 0)

    def outer_early(b, carry):
        ks = [b * pair + g for g in range(pair)]
        parts = []
        for k in ks:
            sides = []
            for s in range(2):
                for o in ((0, 1) if s == 0 else (1, 0)):
                    at = lax.broadcasted_iota(jnp.int32, (ch, levels), 0)
                    sides.append(jnp.where(at == ch - 1, 0.0, gr[o, s, k]))
                    sides.append(gr[2, s, k] if o == 0 else jnp.zeros((ch, levels), F32))
            parts.append(jnp.concatenate(sides, axis=0))
        back = dot(em[...], jnp.concatenate(split2(jnp.concatenate(parts, axis=1)), axis=0))
        hi, lo = split2(back)
        for g, k in enumerate(ks):
            part = slice(g * levels, (g + 1) * levels)
            both = jnp.concatenate([hi[:, part], lo[:, part]], axis=1)
            add = dot(both, lv_nn).reshape(4, cols, levels)
            out[k, 0:2] += add[0:2]
            out[k, rows - 2 : rows] += add[2:4]
        return carry

    for c in order[:1]:
        second.forward(3, c)
    second.receive(0)
    third = steps // 3
    lax.fori_loop(0, third, outer_early, 0)
    for c in order[1:2]:
        second.forward(3, c)
    lax.fori_loop(third, 2 * third, outer_early, 0)
    for c in order[2:]:
        second.forward(3, c)
    lax.fori_loop(2 * third, steps, outer_early, 0)

    for s in range(2):
        @pl.when(has[s])
        def _(s=s):
            remote(gr15.at[s], gr15.at[s], g15_s.at[s], g15_r.at[s], m, near[s]).wait_recv()
    blank = jnp.zeros((12, levels), F32)

    def outer_late(c):
        ks = list(range(c * per, (c + 1) * per))
        rowsets = []
        for k in ks:
            rowsets += [gr[3, 0, k], gr[3, 1, k]] + [gr15[s, w, k : k + 1] for s in range(2) for w in range(2)] + [blank]
        both = jnp.concatenate(split2(jnp.concatenate(rowsets, axis=0)), axis=1)
        hi, lo = split2(dot(both, lv_nn))
        span = 2 * ch + 16
        stack = jnp.concatenate(
            [jnp.concatenate([x[g * span : (g + 1) * span] for g in range(len(ks))], axis=1) for x in (hi, lo)], axis=0)
        add = dot(el[...], stack)
        for g, k in enumerate(ks):
            piece = add[:, g * levels : (g + 1) * levels].reshape(4, cols, levels)
            out[k, 0:2] += piece[0:2]
            out[k, rows - 2 : rows] += piece[2:4]

    mixed = order[1:-1][::-1] + [0] + order[:1] if chunks > 1 else order
    for c in mixed:
        second.receive_chunk(3, c)
        outer_late(c)

    first.drain()
    second.drain()
    for g in range(3):
        to_mate(g).wait_send()
        for d in range(1, n // 2):
            to_peer(g, d).wait_send()
        back_to_mate(g).wait_send()
    for h in range(2):
        for s in range(2):
            @pl.when(has[s] & (p == s))
            def _(h=h, s=s):
                for d in range(n // 2):
                    outer_copy(h, s, d).wait_send()

            @pl.when(has[s] & (p == s))
            def _(h=h, s=s):
                edge_copy(h, s).wait_send()

            @pl.when(has[s] & (p == 1 - s))
            def _(h=h, s=s):
                hand_over(h, s).wait_send()
    for s in range(2):
        @pl.when(has[s])
        def _(s=s):
            single_copy(adjs15, ahalo15, a15_s, a15_r, s).wait_send()
            single_copy(gs15, gr15, g15_s, g15_r, s).wait_send()


def solution(mesh):
    n = mesh.shape["mem"]
    tiles = mesh.shape["tile"]

    def on_device(alpha, ensemble, loc_vert, obs_col, obs_lev, obs_count, innovation, obs_weight):
        members, rows, cols, levels = alpha.shape
        slots = obs_col.shape[1]
        chunks = 4 if members % 4 == 0 else 1
        ch = cols // 2
        mid = (rows - 4) // 2
        vmem = pl.BlockSpec(memory_space=pltpu.VMEM)
        hbm = pl.BlockSpec(memory_space=pltpu.HBM)
        turned = pltpu.VMEM((2, 2, members, 2, ch, levels), F32)
        passing = pltpu.VMEM((2, members, 2, ch, levels), F32)
        line2 = pltpu.VMEM((4, 2, members, ch, levels), F32)
        passing2 = pltpu.VMEM((4, members, ch, levels), F32)
        dma = pltpu.SemaphoreType.DMA
        line = pltpu.VMEM((1, slots), F32)
        mark = pltpu.VMEM((1, slots), jnp.int32)
        padded = -(-members // 8) * 8
        thin = -(-6 * V // 16) * 16

        def sums(piece, result):
            return [pltpu.VMEM((2,) + piece, F32), pltpu.VMEM(piece, F32),
                    pltpu.VMEM((max(n // 2 - 1, 1),) + piece, F32), pltpu.VMEM((2,) + result, F32)]

        borders = pltpu.VMEM((2, 2, V, ch, levels), F32)
        small = pltpu.VMEM((2, 8, levels), F32)
        slim = pltpu.VMEM((2, 2, padded, levels), F32)
        return pl.pallas_call(
            functools.partial(kernel, n, tiles, chunks),
            out_shape=jax.ShapeDtypeStruct(alpha.shape, F32),
            in_specs=[hbm, hbm, hbm, hbm, hbm, pl.BlockSpec(memory_space=pltpu.SMEM), hbm, hbm],
            out_specs=vmem,
            scratch_shapes=[
                pltpu.VMEM(alpha.shape, BF16), pltpu.VMEM(ensemble.shape, BF16),
                pltpu.VMEM(loc_vert.shape, BF16), mark, mark, line, line,
                turned, turned, passing, line2, line2, passing2,
                pltpu.VMEM((rows * cols, rows * cols), BF16),
                pltpu.VMEM((4 * cols, 4 * cols), BF16),
                pltpu.VMEM((4 * cols, 8 * cols), BF16),
                pltpu.VMEM((4 * cols, 4 * ch + 32), BF16),
                pltpu.VMEM((2, thin + V * (rows + 2) * ch, slots), BF16),
                pltpu.VMEM((thin, slots), F32),
                pltpu.VMEM((2 * levels, slots), BF16),
                pltpu.VMEM((2, 2, V, padded, levels), F32),
                *sums((V, mid, cols, levels), (V, mid, cols, levels)),
                *sums((V, 2, ch, levels), (V, 3, ch, levels)), *sums((V, 2, ch, levels), (V, 3, ch, levels)),
                pltpu.VMEM((2, n // 2, V, ch, levels), F32), pltpu.VMEM((V, rows, cols, levels), F32), borders, borders,
                small, small, slim, slim,
                dma((9,)),
                dma((2,)), dma((2, 2)), dma((1,)), dma((2, chunks)),
                dma((2,)), dma((1, 2)), dma((2, chunks)), dma((1,)), dma((4, chunks)),
                dma((3, n // 2 + 1)), dma((3, n // 2 + 1)),
                dma((2, n // 2)), dma((2, n // 2)), dma((2,)), dma((2, 2)), dma((2,)),
                dma((2,)), dma((2,)), dma((2,)), dma((2,)),
            ],
            compiler_params=pltpu.CompilerParams(
                collective_id=0, has_side_effects=True, vmem_limit_bytes=48 << 20),
        )(*[pltpu.with_memory_space_constraint(x, pltpu.HBM) for x in (alpha, ensemble, loc_vert, obs_col, obs_lev)],
          obs_count, *[pltpu.with_memory_space_constraint(x, pltpu.HBM) for x in (innovation, obs_weight)])

    in_specs = (
        P("mem", "tile", None, None),
        P("mem", None, "tile", None, None),
        P(),
        P("tile", None),
        P("tile", None),
        P("tile"),
        P("tile", None),
        P("tile", None),
    )
    out_specs = P("mem", "tile", None, None)
    return jax.shard_map(
        on_device, mesh=mesh, in_specs=in_specs, out_specs=out_specs, check_vma=False
    )
```

```python
import functools

import jax
import jax.numpy as jnp
from jax import lax
from jax.experimental import pallas as pl
from jax.experimental.pallas import tpu as pltpu
from jax.sharding import PartitionSpec as P

V = 3
F32 = jnp.float32
BF16 = jnp.bfloat16
MESH = pl.DeviceIdType.MESH


def split2(x):
    hi = x.astype(BF16)
    lo = (x - hi.astype(F32)).astype(BF16)
    return hi, lo


def dot(a, b):
    return jnp.dot(a, b, preferred_element_type=F32)


def dot_nt(a, b):
    return lax.dot_general(a, b, (((1,), (1,)), ((), ())), preferred_element_type=F32)


def band(distance):
    d = jnp.abs(distance)
    return jnp.where(d == 0, 6.0, jnp.where(d == 1, 4.0, jnp.where(d == 2, 1.0, 0.0)))


def column_weight(c, c2, cols):
    end = (c == c2) & ((c == 0) | (c == cols - 1))
    return (band(c - c2) - jnp.where(end, 1.0, 0.0)) * (1.0 / 16.0)


def kernel(n, tiles, chunks, alpha_h, ens_h, loc_h, col_h, lev_h, cnt, innov_h, wgt_h, out,
           av, ens, loc, col, lev, innov, wgt,
           hs, hr, hl, gs, gr, gl, mm, sc, em, el, wt, w15, sent, e15,
           bi, bi1, bi2, fi, b0, b01, b02, f0, b1, b11, b12, f1,
           iy, adj, adjs, ahalo, adjs15, ahalo15, gs15, gr15,
           in_sem, hs_s, hs_r, hl_s, hl_r, gs_s, gs_r, ge_r, gl_s, gl_r,
           sh_s, sh_r, ih_s, ih_r, ah_s, ah_r, ah_f, a15_s, a15_r, g15_s, g15_r):
    members, rows, cols, levels = out.shape
    size = rows * cols
    ch = cols // 2
    mid = (rows - 4) // 2
    per = members // chunks
    group = 4 if members % 4 == 0 else 1
    slots = col.shape[1]
    m = lax.axis_index("mem")
    t = lax.axis_index("tile")
    p = lax.rem(m, 2)
    mate = m + 1 - 2 * p
    has = (t > 0, t < tiles - 1)
    near = (t - 1, t + 1)
    edge = (slice(0, 2), slice(rows - 2, rows))
    half = (slice(0, ch), slice(ch, cols))

    def loads():
        pairs = (
            (alpha_h.at[:, 0:2], av.at[:, 0:2]),
            (alpha_h.at[:, rows - 2 : rows], av.at[:, rows - 2 : rows]),
            (loc_h, loc),
            (alpha_h.at[:, 2 : rows - 2], av.at[:, 2 : rows - 2]),
            (ens_h, ens),
            (col_h, col), (lev_h, lev), (innov_h, innov), (wgt_h, wgt))
        return [pltpu.make_async_copy(a, b, in_sem.at[i]) for i, (a, b) in enumerate(pairs)]

    copies = loads()
    for copy in copies:
        copy.start()

    relays = tiles % 2 == 0 and tiles >= 4
    lead = chunks // 2
    odd = lax.rem(t, 2)
    turn = tiles // 2
    share_out = lax.div(chunks * lax.div(t + odd, 2), max(turn, 1))
    n_out = odd * (chunks - share_out) + (1 - odd) * share_out
    share_in = lax.div(chunks * lax.div(t + 2 - 3 * odd, 2), max(turn, 1))
    n_in = (1 - odd) * (chunks - share_in) + odd * share_in
    far = (t >= 2, t <= tiles - 3)
    passes = jnp.where(odd == 1, t - 2, tiles - 3 - t) >= 0

    barrier = pltpu.get_barrier_semaphore()

    def greet(who, where):
        pl.semaphore_signal(barrier, inc=1, device_id={"mem": who, "tile": where}, device_id_type=MESH)

    for d in range(1, n):
        greet(lax.rem(m + d, n), t)
    total = jnp.int32(n - 1)
    for s in range(2):
        @pl.when(has[s])
        def _(s=s):
            for d in range(n // 2):
                greet(lax.rem(m + 2 * d, n), near[s])
        total = total + (n // 2) * has[s].astype(jnp.int32)
        if relays:
            @pl.when(far[s])
            def _(s=s):
                greet(m, t - 2 + 4 * s)
            total = total + far[s].astype(jnp.int32)

    def remote(src, dst, ssem, rsem, who, where):
        return pltpu.make_async_remote_copy(
            src_ref=src, dst_ref=dst, send_sem=ssem, recv_sem=rsem,
            device_id={"mem": who, "tile": where}, device_id_type=MESH)

    class Halo:
        def __init__(self, src, dst, via, ss, sr, vs, vr, groups, fine=None):
            self.src, self.dst, self.via = src, dst, via
            self.ss, self.sr, self.vs, self.vr = ss, sr, vs, vr
            self.groups, self.fine = groups, fine

        def group(self, h):
            return [b for b, span in enumerate(self.groups) if span[0] <= h < span[1]][0]

        def landed(self, h, s, c):
            if self.fine is not None and h == self.src.shape[0] - 1:
                return self.fine.at[s, c]
            return self.sr.at[self.group(h), s]

        def direct(self, h, s, c):
            part = pl.ds(c * per, per)
            return remote(self.src.at[h, s, part], self.dst.at[h, 1 - s, part],
                          self.ss.at[s], self.landed(h, 1 - s, c), m, near[s])

        def receive_chunk(self, h, c):
            for s in range(2):
                @pl.when(has[s])
                def _(s=s):
                    part = self.dst.at[h, s, pl.ds(c * per, per)]
                    remote(part, part, self.ss.at[s], self.landed(h, s, c), m, near[s]).wait_recv()

        def detour(self, h, s, c):
            part = pl.ds(c * per, per)
            return remote(self.src.at[h, s, part], self.via.at[h, part],
                          self.ss.at[s], self.vr.at[h, c], m, t + 1 - 2 * odd)

        def onward(self, h, c):
            part = pl.ds(c * per, per)
            return remote(self.via.at[h, part], self.dst.at[h, odd, part],
                          self.vs.at[0], self.landed(h, odd, c), m, t + 2 - 4 * odd)

        def send_turned(self, h, c):
            for s in range(2):
                if relays:
                    @pl.when(has[s] & (odd == s) & (c >= chunks - n_out))
                    def _(s=s):
                        self.detour(h, s, c).start()

        def send_far(self, h, c):
            for s in range(2):
                straight = c < chunks - n_out if relays else True

                @pl.when(has[s] & (odd == s) & straight)
                def _(s=s):
                    self.direct(h, s, c).start()

        def send_near(self, h, c, when=True):
            for s in range(2):
                @pl.when(has[s] & (odd != s) & when)
                def _(s=s):
                    self.direct(h, s, c).start()

        def send_close(self, h):
            for c in order:
                self.send_turned(h, c)
            for c in order:
                self.send_near(h, c)

        def forward(self, h, c):
            if relays:
                @pl.when(passes & (c >= chunks - n_in))
                def _():
                    self.onward_recv(h, c).wait_recv()
                    self.onward(h, c).start()

        def onward_recv(self, h, c):
            part = pl.ds(c * per, per)
            return remote(self.via.at[h, part], self.via.at[h, part],
                          self.vs.at[0], self.vr.at[h, c], m, t + 1 - 2 * odd)

        def receive(self, b):
            span = self.groups[b]
            for s in range(2):
                @pl.when(has[s])
                def _(s=s):
                    every = self.dst.at[span[0] : span[1], s]
                    remote(every, every, self.ss.at[s], self.sr.at[b, s], m, near[s]).wait_recv()

        def drain(self):
            for s in range(2):
                @pl.when(has[s])
                def _(s=s):
                    remote(self.src.at[:, s], self.dst.at[:, s], self.ss.at[s], self.sr.at[0, s], m, near[s]).wait_send()
            if relays:
                for count in range(1, chunks + 1):
                    @pl.when(passes & (n_in == count))
                    def _(count=count):
                        every = self.via.at[:, members - count * per : members]
                        remote(every, every, self.vs.at[0], self.sr.at[0, 0], m, t + 2 - 4 * odd).wait_send()

    first = Halo(hs, hr, hl, hs_s, hs_r, hl_s, hl_r, ((0, 1), (1, 2)))
    second = Halo(gs, gr, gl, gs_s, gs_r, gl_s, gl_r, ((0, 3),), ge_r)
    order = list(range(chunks - 1, -1, -1))

    i = lax.broadcasted_iota(jnp.int32, (4 * cols, 4 * cols), 0)
    j = lax.broadcasted_iota(jnp.int32, (4 * cols, 4 * cols), 1)
    q, q2 = lax.div(i, cols), lax.div(j, cols)
    across = column_weight(i - q * cols, j - q2 * cols, cols)
    sc[...] = (jnp.where(q == q2, 1.0 / 16.0, 0.0) * across).astype(BF16)
    r = jnp.where(q < 2, q, q + rows - 4)
    r2 = jnp.where(q2 < 2, q2 - 2, q2 - 2 + rows)
    corner = (band(r - r2) * (1.0 / 16.0) * across).astype(BF16)
    em[:, 0 : 4 * cols] = corner
    em[:, 4 * cols :] = corner

    for k in range(3):
        copies[k].wait()
    lv = loc[...]
    lv_nt = jnp.concatenate([lv, lv], axis=1)
    lv_nn = jnp.concatenate([lv, lv], axis=0)

    def prepare(k):
        x = jnp.concatenate([av[k, 0:2], av[k, rows - 2 : rows]], axis=0).reshape(4 * cols, levels)
        both = jnp.concatenate(split2(dot(sc[...], x)), axis=1)
        u = dot_nt(both, lv_nt).reshape(4, cols, levels)
        for s in range(2):
            for h in range(2):
                hs[h, s, k] = u[2 * s : 2 * s + 2, half[h]]

    for c in order:
        for k in range(c * per, (c + 1) * per):
            prepare(k)
        if c == order[0]:
            pl.semaphore_wait(barrier, total)
        first.send_turned(0, c)
        first.send_far(0, c)
        if c != order[0]:
            first.send_near(0, c + 1)
    first.send_near(0, order[-1])
    for c in order:
        first.send_turned(1, c)
    ahead = [(chunks - c) + n_out <= lead for c in range(chunks)]
    for c in order:
        first.send_near(1, c, ahead[c])
    for s in range(2):
        @pl.when(jnp.logical_not(has[s]))
        def _(s=s):
            for ref in (hr, gr, ahalo):
                for h in range(ref.shape[0]):
                    ref[h, s] = jnp.zeros(ref.shape[2:], F32)
            ahalo15[s] = jnp.zeros(ahalo15.shape[1:], F32)
            gr15[s] = jnp.zeros(gr15.shape[1:], F32)

    i = lax.broadcasted_iota(jnp.int32, (size, size), 0)
    j = lax.broadcasted_iota(jnp.int32, (size, size), 1)
    r, r2 = lax.div(i, cols), lax.div(j, cols)
    end = (r == r2) & (((r == 0) & (t == 0)) | ((r == rows - 1) & (t == tiles - 1)))
    row_weight = (band(r - r2) - jnp.where(end, 1.0, 0.0)) * (1.0 / 16.0)
    mm[...] = (row_weight * column_weight(i - r * cols, j - r2 * cols, cols)).astype(BF16)

    stage_refs = ((b0, b01, b02, f0), (b1, b11, b12, f1), (bi, bi1, bi2, fi))
    for ref in (b0, b1, bi):
        ref[...] = jnp.zeros_like(ref)
    copies[3].wait()
    copies[4].wait()

    def lift(b, carry):
        ks = [b * group + g for g in range(group)]
        x = jnp.concatenate([av[k].reshape(size, levels) for k in ks], axis=1)
        hi, lo = split2(dot(mm[...], x))
        bases = []
        for g in range(group):
            part = slice(g * levels, (g + 1) * levels)
            both = jnp.concatenate([hi[:, part], lo[:, part]], axis=1)
            bases.append(dot_nt(both, lv_nt).reshape(rows, cols, levels))
        for v in range(V):
            total = ens[ks[0], v].astype(F32) * bases[0]
            for g in range(1, group):
                total = total + ens[ks[g], v].astype(F32) * bases[g]
            for s in range(2):
                bi[s, v] += total[2 + s * mid : 2 + (s + 1) * mid]
                b0[s, v] += total[edge[s], half[0]]
                b1[s, v] += total[edge[s], half[1]]
        return carry

    lax.fori_loop(0, members // group, lift, 0)

    def to_mate(g):
        part, rec, rec2, full = stage_refs[g]
        return remote(part.at[1 - p], rec, sh_s.at[g, 0], sh_r.at[g, 0], mate, t)

    def to_peer(g, d):
        part, rec, rec2, full = stage_refs[g]
        return remote(part.at[p], rec2.at[d - 1], sh_s.at[g, d], sh_r.at[g, d], lax.rem(m + 2 * d, n), t)

    def back_to_mate(g):
        part, rec, rec2, full = stage_refs[g]
        return remote(full.at[p], full.at[p], sh_s.at[g, n // 2], sh_r.at[g, n // 2], mate, t)

    def back_from_mate(g):
        part, rec, rec2, full = stage_refs[g]
        return remote(full.at[1 - p], full.at[1 - p], sh_s.at[g, n // 2], sh_r.at[g, n // 2], mate, t)

    def reduce_chip(g):
        part, rec, rec2, full = stage_refs[g]
        to_mate(g).wait_recv()
        part[p] += rec[...]
        for d in range(1, n // 2):
            to_peer(g, d).start()

    def reduce_rest(g):
        part, rec, rec2, full = stage_refs[g]
        total = part[p]
        for d in range(1, n // 2):
            to_peer(g, d).wait_recv()
            total = total + rec2[d - 1]
        return total

    def outer_copy(h, s, d):
        here = lax.div(m, 2)
        return remote(stage_refs[h][0].at[p, :, s], iy.at[h, here], ih_s.at[h, d], ih_r.at[h, here],
                      lax.rem(m + 2 * d, n), near[s])

    def outer_send(h):
        for s in range(2):
            @pl.when(has[s] & (p == s))
            def _(s=s):
                for d in range(n // 2):
                    outer_copy(h, s, d).start()

    def outer_recv(h):
        full = stage_refs[h][3]
        for s in range(2):
            @pl.when(has[1 - s] & (p == s))
            def _(s=s):
                total = None
                for d in range(n // 2):
                    remote(iy.at[h, d], iy.at[h, d], ih_s.at[h, 0], ih_r.at[h, d], m, near[1 - s]).wait_recv()
                    total = iy[h, d] if total is None else total + iy[h, d]
                full[s, :, 2] = total

            @pl.when(jnp.logical_not(has[1 - s]) & (p == s))
            def _(s=s):
                full[s, :, 2] = jnp.zeros(full.shape[1:2] + full.shape[3:], F32)

    to_mate(2).start()
    first.forward(0, order[0])
    for k in range(5, 9):
        copies[k].wait()

    place = col[...]
    wide = 2 * cols
    frow = lax.div(place, wide)
    fcol = place - frow * wide
    slot = lax.broadcasted_iota(jnp.int32, (1, slots), 1)
    variable = lax.rem(slot, V)
    early = fcol <= 2 * (ch - 1)
    live = slot < cnt[0]

    def weights(fine, count, shift):
        main = lax.div(fine, 2)
        other = jnp.where(fine - 2 * main == 1, main + 1, main - 1)
        at = lax.broadcasted_iota(jnp.int32, (count, slots), 0) - shift
        return jnp.where(at == main, 0.75, 0.0) + jnp.where(at == other, 0.25, 0.0)

    wr = weights(frow, rows + 2, 1)
    wc = weights(fcol, cols, 0)
    head = w15.shape[0]
    w15[...] = jnp.zeros_like(w15)
    rim = [0, 1, 2, rows - 1, rows, rows + 1]
    lines = rim + list(range(3, rows - 1))
    cut = head + len(rim) * V * ch
    for v in range(V):
        mask = jnp.where(variable == v, 1.0, 0.0)
        for b, a in enumerate(lines):
            start = head + (b * V + v) * ch
            line = wr[a : a + 1, :] * mask
            for h in range(2):
                wt[h, start : start + ch, :] = (wc[half[h]] * line).astype(BF16)
            if b < len(rim):
                w15[b * V + v : b * V + v + 1, :] = wc[ch - 1 : ch] * line
        if v == 0:
            reduce_chip(2)
    wt[1, 0:head, :] = w15[...].astype(BF16)
    for c in order[1:2]:
        first.forward(0, c)
    fi[p] = reduce_rest(2)
    back_to_mate(2).start()

    i = lax.broadcasted_iota(jnp.int32, (4 * cols, 2 * ch + 16), 0)
    j = lax.broadcasted_iota(jnp.int32, (4 * cols, 2 * ch + 16), 1)
    q = lax.div(i, cols)
    r = jnp.where(q < 2, q, q + rows - 4)
    spot = j - 2 * ch
    r2 = jnp.where(spot < 0, jnp.where(j < ch, -1, rows), jnp.where(spot < 2, spot - 2, spot - 2 + rows))
    c2 = jnp.where(spot < 0, jnp.where(j < ch, j, j - ch) + ch, ch - 1)
    last = band(r - r2) * (1.0 / 16.0) * column_weight(i - q * cols, c2, cols)
    last = jnp.where(spot < 4, last, 0.0).astype(BF16)
    el[:, 0 : 2 * ch + 16] = last
    el[:, 2 * ch + 16 :] = last

    e15[...] = jnp.zeros_like(e15)
    for s in range(2):
        for w in range(2):
            row = s * (rows - 2) + w
            for v in range(V):
                for k in range(members):
                    e15[s, w, v, k : k + 1, :] = ens[k, v, row, ch - 1 : ch, :].astype(F32)

    def edge_increment(h, c):
        part = stage_refs[h][0]
        sums = [[None] * V for _ in range(2)]
        for k in range(c * per, (c + 1) * per):
            above, below = hr[h, 0, k], hr[h, 1, k]
            fields = (jnp.stack([above[0] + 4.0 * above[1], above[1]]),
                      jnp.stack([below[0], 4.0 * below[0] + below[1]]))
            for s in range(2):
                for v in range(V):
                    term = ens[k, v, edge[s], half[h]].astype(F32) * fields[s]
                    sums[s][v] = term if sums[s][v] is None else sums[s][v] + term
        for s in range(2):
            for v in range(V):
                part[s, v] += sums[s][v]

    hot = lax.broadcasted_iota(jnp.int32, (levels, slots), 0) == lev[...]

    def pick(h, pieces, start):
        flat = jnp.concatenate(pieces, axis=0).reshape(-1, levels)
        both = jnp.concatenate(split2(flat.T), axis=0)
        picked = dot(both, wt[h, start : start + flat.shape[0]])
        return jnp.sum(jnp.where(hot, picked[:levels] + picked[levels:], 0.0), axis=0, keepdims=True)

    def pick_inner(h):
        return pick(h, [fi[s, :, a, half[h]] for s in range(2) for a in range(mid)], cut)

    def pick_rim(h):
        full = stage_refs[h][3]
        return pick(h, [full[1, :, 2], full[0, :, 0], full[0, :, 1], full[1, :, 0], full[1, :, 1], full[0, :, 2]], head)

    def spread(weighted):
        hi, lo = split2(jnp.where(hot, jnp.broadcast_to(weighted, hot.shape), 0.0))
        sent[0:levels, :] = hi
        sent[levels:, :] = lo

    def adjoint(h, start, stop):
        both = dot_nt(wt[h, start:stop, :], sent[...])
        return both[:, :levels] + both[:, levels:]

    def shaped(x):
        return x.reshape(x.shape[0] // (V * ch), V, ch, levels)

    def edge_copy(h, s):
        return remote(adjs.at[h, s], ahalo.at[h, 1 - s], ah_s.at[h], ah_r.at[h, 1 - s], m, near[s])

    def hand_over(h, s):
        return remote(ahalo.at[h, s], ahalo.at[h, s], ah_f.at[h], ah_r.at[h, s], mate, t)

    def single_copy(src, dst, ssem, rsem, s):
        return remote(src.at[s], dst.at[1 - s], ssem.at[s], rsem.at[1 - s], m, near[s])

    def adjoint_edges(h):
        flat = adjoint(h, head * (1 - h), cut)
        thin = flat[:head] if h else None
        rims = shaped(flat[head * h :])
        adjs[h, 0] = rims[0]
        adjs[h, 1] = rims[5]
        if h:
            adjs15[0, 0:V] = thin[0:V]
            adjs15[1, 0:V] = thin[5 * V : 6 * V]
        for s in range(2):
            @pl.when(has[s] & (p == s))
            def _(s=s):
                edge_copy(h, s).start()

            @pl.when(has[s])
            def _(s=s):
                if h:
                    single_copy(adjs15, ahalo15, a15_s, a15_r, s).start()
        for a in range(2):
            adj[:, a, half[h]] = rims[1 + a]
            adj[:, rows - 2 + a, half[h]] = rims[3 + a]
        return thin

    def adjoint_halo(h):
        for s in range(2):
            @pl.when(has[s] & (p == 1 - s))
            def _(s=s):
                hand_over(h, s).wait_recv()
                hand_over(h, s).start()
        for s in range(2):
            @pl.when(has[s] & (p == s))
            def _(s=s):
                hand_over(h, s).wait_recv()
        adj[:, 0, half[h]] += ahalo[h, 0]
        adj[:, rows - 1, half[h]] += ahalo[h, 1]

    def fields(h, outermost):
        where = (0, rows - 1) if outermost else (1, rows - 2)
        weights = [[adj[v, where[s], half[h]] for v in range(V)] for s in range(2)]
        for k in range(members):
            for s in range(2):
                total = ens[k, 0, where[s], half[h]].astype(F32) * weights[s][0]
                for v in range(1, V):
                    total = total + ens[k, v, where[s], half[h]].astype(F32) * weights[s][v]
                gs[2 * h + outermost, s, k] = total

    def chain_open(h):
        first.receive(h)
        for c in order:
            edge_increment(h, c)
        to_mate(h).start()
        reduce_chip(h)
        outer_send(h)

    def chain_close(h, between, after):
        full = stage_refs[h][3]
        full[p, :, 0:2] = reduce_rest(h)
        between()
        outer_recv(h)
        back_to_mate(h).start()
        after()
        back_from_mate(h).wait_recv()

    back_from_mate(2).wait_recv()
    value = pick_inner(0)
    for c in order[2:]:
        first.forward(0, c)
    value = value + pick_inner(1)

    def release(halo, h):
        for c in order:
            halo.send_far(h, c)

    def between_a():
        release(first, 1)
        first.forward(1, order[0])

    chain_open(0)
    for c in order:
        first.send_near(1, c, jnp.logical_not(ahead[c]))
    chain_close(0, between_a, lambda: None)
    for c in order[1:2]:
        first.forward(1, c)
    value = value + pick_rim(0)
    weighted = jnp.where(live & early, wgt[...] * (value - innov[...]), 0.0)
    spread(weighted)
    adjoint_edges(0)
    fields(0, 0)
    early_near = [(chunks - c) + n_out <= chunks for c in range(chunks)]
    for c in order:
        second.send_turned(0, c)
    for c in order:
        second.send_near(0, c, early_near[c])
    for c in order[2:]:
        first.forward(1, c)

    chain_open(1)
    for c in order:
        second.send_near(0, c, jnp.logical_not(early_near[c]))
    adjoint_halo(0)
    fields(0, 1)
    second.send_close(1)
    for c in order[:2]:
        second.forward(0, c)
    chain_close(1, lambda: release(second, 0), lambda: release(second, 1))
    for c in order[2:]:
        second.forward(0, c)
    value = value + pick_rim(1)
    spread(jnp.where(live, wgt[...] * (value - innov[...]), 0.0))
    thin = adjoint_edges(1)
    fields(1, 0)
    second.send_close(2)
    for c in order:
        second.forward(1, c)
    for h in range(2):
        inner = shaped(adjoint(h, cut, wt.shape[1]))
        for a in range(rows - 4):
            adj[:, 2 + a, half[h]] = inner[a]
    adjoint_halo(1)
    for s in range(2):
        @pl.when(has[s])
        def _(s=s):
            remote(ahalo15.at[s], ahalo15.at[s], a15_s.at[s], a15_r.at[s], m, near[s]).wait_recv()
    for s in range(2):
        for w in range(2):
            a = 1 + 2 * s + w
            line = thin[a * V : (a + 1) * V]
            if w == s:
                line = line + ahalo15[s, 0:V]
            total = e15[s, w, 0] * line[0:1]
            for v in range(1, V):
                total = total + e15[s, w, v] * line[v : v + 1]
            gs15[s, w] = total
            for v in range(V):
                adj[v, s * (rows - 2) + w, ch - 1 : ch, :] = line[v : v + 1]
    for s in range(2):
        @pl.when(has[s])
        def _(s=s):
            single_copy(gs15, gr15, g15_s, g15_r, s).start()
    fields(1, 1)
    for c in order:
        second.send_far(2, c)
    second.send_close(3)
    for c in order:
        second.send_far(3, c)

    pair = group

    def inside(b, carry):
        ks = [b * pair + g for g in range(pair)]
        parts = []
        for k in ks:
            total = ens[k, 0].astype(F32) * adj[0]
            for v in range(1, V):
                total = total + ens[k, v].astype(F32) * adj[v]
            parts.append(total.reshape(size, levels))
        hi, lo = split2(jnp.concatenate(parts, axis=1))
        hi, lo = split2(dot(mm[...], hi) + dot(mm[...], lo))
        for g, k in enumerate(ks):
            part = slice(g * levels, (g + 1) * levels)
            both = jnp.concatenate([hi[:, part], lo[:, part]], axis=1)
            out[k] = av[k].astype(F32) + dot(both, lv_nn).reshape(rows, cols, levels)
        return carry

    steps = members // pair
    stops = [0, steps // 5, 2 * steps // 5, steps]
    lax.fori_loop(stops[0], stops[1], inside, 0)
    for c in order[:2]:
        second.forward(2, c)
    lax.fori_loop(stops[1], stops[2], inside, 0)
    for c in order[2:]:
        second.forward(2, c)
    lax.fori_loop(stops[2], stops[3], inside, 0)

    def outer_early(b, carry):
        ks = [b * pair + g for g in range(pair)]
        parts = []
        for k in ks:
            sides = []
            for s in range(2):
                for o in ((0, 1) if s == 0 else (1, 0)):
                    at = lax.broadcasted_iota(jnp.int32, (ch, levels), 0)
                    sides.append(jnp.where(at == ch - 1, 0.0, gr[o, s, k]))
                    sides.append(gr[2, s, k] if o == 0 else jnp.zeros((ch, levels), F32))
            parts.append(jnp.concatenate(sides, axis=0))
        back = dot(em[...], jnp.concatenate(split2(jnp.concatenate(parts, axis=1)), axis=0))
        hi, lo = split2(back)
        for g, k in enumerate(ks):
            part = slice(g * levels, (g + 1) * levels)
            both = jnp.concatenate([hi[:, part], lo[:, part]], axis=1)
            add = dot(both, lv_nn).reshape(4, cols, levels)
            out[k, 0:2] += add[0:2]
            out[k, rows - 2 : rows] += add[2:4]
        return carry

    for c in order[:1]:
        second.forward(3, c)
    second.receive(0)
    third = steps // 3
    lax.fori_loop(0, third, outer_early, 0)
    for c in order[1:2]:
        second.forward(3, c)
    lax.fori_loop(third, 2 * third, outer_early, 0)
    for c in order[2:]:
        second.forward(3, c)
    lax.fori_loop(2 * third, steps, outer_early, 0)

    for s in range(2):
        @pl.when(has[s])
        def _(s=s):
            remote(gr15.at[s], gr15.at[s], g15_s.at[s], g15_r.at[s], m, near[s]).wait_recv()
    blank = jnp.zeros((12, levels), F32)

    def outer_late(c):
        ks = list(range(c * per, (c + 1) * per))
        rowsets = []
        for k in ks:
            rowsets += [gr[3, 0, k], gr[3, 1, k]] + [gr15[s, w, k : k + 1] for s in range(2) for w in range(2)] + [blank]
        both = jnp.concatenate(split2(jnp.concatenate(rowsets, axis=0)), axis=1)
        hi, lo = split2(dot(both, lv_nn))
        span = 2 * ch + 16
        stack = jnp.concatenate(
            [jnp.concatenate([x[g * span : (g + 1) * span] for g in range(len(ks))], axis=1) for x in (hi, lo)], axis=0)
        add = dot(el[...], stack)
        for g, k in enumerate(ks):
            piece = add[:, g * levels : (g + 1) * levels].reshape(4, cols, levels)
            out[k, 0:2] += piece[0:2]
            out[k, rows - 2 : rows] += piece[2:4]

    mixed = order[1:-1][::-1] + order[:1] + [0] if chunks > 1 else order
    for c in mixed:
        second.receive_chunk(3, c)
        outer_late(c)

    first.drain()
    second.drain()
    for g in range(3):
        to_mate(g).wait_send()
        for d in range(1, n // 2):
            to_peer(g, d).wait_send()
        back_to_mate(g).wait_send()
    for h in range(2):
        for s in range(2):
            @pl.when(has[s] & (p == s))
            def _(h=h, s=s):
                for d in range(n // 2):
                    outer_copy(h, s, d).wait_send()

            @pl.when(has[s] & (p == s))
            def _(h=h, s=s):
                edge_copy(h, s).wait_send()

            @pl.when(has[s] & (p == 1 - s))
            def _(h=h, s=s):
                hand_over(h, s).wait_send()
    for s in range(2):
        @pl.when(has[s])
        def _(s=s):
            single_copy(adjs15, ahalo15, a15_s, a15_r, s).wait_send()
            single_copy(gs15, gr15, g15_s, g15_r, s).wait_send()


def solution(mesh):
    n = mesh.shape["mem"]
    tiles = mesh.shape["tile"]

    def on_device(alpha, ensemble, loc_vert, obs_col, obs_lev, obs_count, innovation, obs_weight):
        members, rows, cols, levels = alpha.shape
        slots = obs_col.shape[1]
        chunks = 4 if members % 4 == 0 else 1
        ch = cols // 2
        mid = (rows - 4) // 2
        vmem = pl.BlockSpec(memory_space=pltpu.VMEM)
        hbm = pl.BlockSpec(memory_space=pltpu.HBM)
        turned = pltpu.VMEM((2, 2, members, 2, ch, levels), F32)
        passing = pltpu.VMEM((2, members, 2, ch, levels), F32)
        line2 = pltpu.VMEM((4, 2, members, ch, levels), F32)
        passing2 = pltpu.VMEM((4, members, ch, levels), F32)
        dma = pltpu.SemaphoreType.DMA
        line = pltpu.VMEM((1, slots), F32)
        mark = pltpu.VMEM((1, slots), jnp.int32)
        padded = -(-members // 8) * 8
        thin = -(-6 * V // 16) * 16

        def sums(piece, result):
            return [pltpu.VMEM((2,) + piece, F32), pltpu.VMEM(piece, F32),
                    pltpu.VMEM((max(n // 2 - 1, 1),) + piece, F32), pltpu.VMEM((2,) + result, F32)]

        borders = pltpu.VMEM((2, 2, V, ch, levels), F32)
        small = pltpu.VMEM((2, 8, levels), F32)
        slim = pltpu.VMEM((2, 2, padded, levels), F32)
        return pl.pallas_call(
            functools.partial(kernel, n, tiles, chunks),
            out_shape=jax.ShapeDtypeStruct(alpha.shape, F32),
            in_specs=[hbm, hbm, hbm, hbm, hbm, pl.BlockSpec(memory_space=pltpu.SMEM), hbm, hbm],
            out_specs=vmem,
            scratch_shapes=[
                pltpu.VMEM(alpha.shape, BF16), pltpu.VMEM(ensemble.shape, BF16),
                pltpu.VMEM(loc_vert.shape, BF16), mark, mark, line, line,
                turned, turned, passing, line2, line2, passing2,
                pltpu.VMEM((rows * cols, rows * cols), BF16),
                pltpu.VMEM((4 * cols, 4 * cols), BF16),
                pltpu.VMEM((4 * cols, 8 * cols), BF16),
                pltpu.VMEM((4 * cols, 4 * ch + 32), BF16),
                pltpu.VMEM((2, thin + V * (rows + 2) * ch, slots), BF16),
                pltpu.VMEM((thin, slots), F32),
                pltpu.VMEM((2 * levels, slots), BF16),
                pltpu.VMEM((2, 2, V, padded, levels), F32),
                *sums((V, mid, cols, levels), (V, mid, cols, levels)),
                *sums((V, 2, ch, levels), (V, 3, ch, levels)), *sums((V, 2, ch, levels), (V, 3, ch, levels)),
                pltpu.VMEM((2, n // 2, V, ch, levels), F32), pltpu.VMEM((V, rows, cols, levels), F32), borders, borders,
                small, small, slim, slim,
                dma((9,)),
                dma((2,)), dma((2, 2)), dma((1,)), dma((2, chunks)),
                dma((2,)), dma((1, 2)), dma((2, chunks)), dma((1,)), dma((4, chunks)),
                dma((3, n // 2 + 1)), dma((3, n // 2 + 1)),
                dma((2, n // 2)), dma((2, n // 2)), dma((2,)), dma((2, 2)), dma((2,)),
                dma((2,)), dma((2,)), dma((2,)), dma((2,)),
            ],
            compiler_params=pltpu.CompilerParams(
                collective_id=0, has_side_effects=True, vmem_limit_bytes=48 << 20),
        )(*[pltpu.with_memory_space_constraint(x, pltpu.HBM) for x in (alpha, ensemble, loc_vert, obs_col, obs_lev)],
          obs_count, *[pltpu.with_memory_space_constraint(x, pltpu.HBM) for x in (innovation, obs_weight)])

    in_specs = (
        P("mem", "tile", None, None),
        P("mem", None, "tile", None, None),
        P(),
        P("tile", None),
        P("tile", None),
        P("tile"),
        P("tile", None),
        P("tile", None),
    )
    out_specs = P("mem", "tile", None, None)
    return jax.shard_map(
        on_device, mesh=mesh, in_specs=in_specs, out_specs=out_specs, check_vma=False
    )
```
